8 devices in a mesh: dp: 2 (over z, y), tp: 4 (over x, core).
Axes of the slice: x: 2, y: 2, z: 1, core: 2. Of those that a mesh axis runs over, the one named last changes fastest.
Arguments:
- y_one: float32 [8, 32, 2048], P('dp'), parts along dimension 0
- y_two: float32 [8, 32, 2048], P('dp'), parts along dimension 0
- dy_one: float32 [8, 32, 2048], P('dp'), parts along dimension 0
- dy_two: float32 [8, 32, 2048], P('dp'), parts along dimension 0
- seq_lens: int32 [8], P('dp'), parts along dimension 0
- w_query: bfloat16 [3, 2048, 32, 64], P(None, None, 'tp')
- w_key: bfloat16 [3, 2048, 8, 64], P(None, None, 'tp')
- w_value: bfloat16 [3, 2048, 8, 64], P(None, None, 'tp')
- w_out: bfloat16 [3, 32, 64, 2048], P(None, 'tp')
- w_up: bfloat16 [3, 2048, 8192], P(None, None, 'tp')
- w_down: bfloat16 [3, 8192, 2048], P(None, 'tp')
Outputs:
- output 1: float32 [8, 32, 2048], P('dp'), parts along dimension 0
- output 2: float32 [8, 32, 2048], P('dp'), parts along dimension 0
- output 3: float32 [8, 32, 2048], P('dp'), parts along dimension 0
- output 4: float32 [8, 32, 2048], P('dp'), parts along dimension 0
- output 5: float32 [6, 2048, 32, 64], P('dp', None, 'tp'), parts along dimension 0
- output 6: float32 [6, 2048, 8, 64], P('dp', None, 'tp'), parts along dimension 0
- output 7: float32 [6, 2048, 8, 64], P('dp', None, 'tp'), parts along dimension 0
- output 8: float32 [6, 32, 64, 2048], P('dp', 'tp'), parts along dimension 0
- output 9: float32 [6, 2048, 8192], P('dp', None, 'tp'), parts along dimension 0
- output 10: float32 [6, 8192, 2048], P('dp', 'tp'), parts along dimension 0
There are 2 independent parts. The reference program is written for one: setup_inputs(seed, part) draws one part's arguments, and reference() takes and returns one part's arrays. A program takes and returns all parts, laid end to end along the dimension named above; an argument that names none is the same for every part.
All inputs are finite; a program needn't handle non-finite values.
Results may differ from the reference program's by a relative error of at most 0.02.
Values are sent between devices in bfloat16 or wider.
A program may use at most 1 GiB of HBM per device.

```python
import functools
import jax
import jax.numpy as jnp
from jax import lax

D = 2048
HEADS = 32
KV_HEADS = 8
HEAD = 64
FF = 8192
LAYERS = 3
SEQS = 1
SEQ = 32
TP = 4
KV_SLOTS = max(KV_HEADS, TP)
REPEAT = KV_SLOTS // KV_HEADS
GROUP = HEADS // KV_SLOTS
BATCH = SEQS * TP
TOKENS = BATCH * SEQ
EPS = 1e-5
SCORE_SCALE = HEAD ** -0.5
OUT_GAIN = 0.5 * (SEQ / 64) ** 0.25


def normal_weights(rng_key, arr_shape, scale_std):
    return (jax.random.normal(rng_key, arr_shape, jnp.float32) * scale_std).astype(jnp.bfloat16)


def draw_lengths(rng_key):
    len_key, top_key, low_key = jax.random.split(rng_key, 3)
    seq_lens = jax.random.randint(len_key, (BATCH,), SEQ // 4, SEQ + 1)
    top_idx = jax.random.randint(top_key, (), 0, BATCH)
    low_idx = (top_idx + jax.random.randint(low_key, (), 1, BATCH)) % BATCH
    positions = jnp.arange(BATCH)
    seq_lens = jnp.where(positions == top_idx, SEQ, seq_lens)
    seq_lens = jnp.where(positions == low_idx, SEQ // 4, seq_lens)
    return seq_lens.astype(jnp.int32)


def setup_inputs(seed: int = 0, part: int = 0) -> dict:
    weight_keys = jax.random.split(jax.random.key(seed), 6)
    part_keys = jax.random.split(jax.random.fold_in(jax.random.key(seed + 1), part), 5)
    act_shape = (BATCH, SEQ, D)
    key_heads = normal_weights(weight_keys[1], (LAYERS, D, KV_HEADS, HEAD), D ** -0.5)
    value_heads = normal_weights(weight_keys[2], (LAYERS, D, KV_HEADS, HEAD), D ** -0.5)
    return {
        'y_one': jax.random.normal(part_keys[0], act_shape, jnp.float32),
        'y_two': jax.random.normal(part_keys[1], act_shape, jnp.float32),
        'dy_one': jax.random.normal(part_keys[2], act_shape, jnp.float32),
        'dy_two': jax.random.normal(part_keys[3], act_shape, jnp.float32),
        'seq_lens': draw_lengths(part_keys[4]),
        'w_query': normal_weights(weight_keys[0], (LAYERS, D, HEADS, HEAD), 2.0 * D ** -0.5),
        'w_key': jnp.repeat(key_heads, REPEAT, axis=2),
        'w_value': jnp.repeat(value_heads, REPEAT, axis=2),
        'w_out': normal_weights(weight_keys[3], (LAYERS, HEADS, HEAD, D), OUT_GAIN * (HEADS * HEAD) ** -0.5),
        'w_up': normal_weights(weight_keys[4], (LAYERS, D, FF), D ** -0.5),
        'w_down': normal_weights(weight_keys[5], (LAYERS, FF, D), 0.6 * FF ** -0.5),
    }


def rms_norm(x_val):
    inv_rms = lax.rsqrt(jnp.mean(x_val * x_val, axis=-1, keepdims=True) + EPS)
    return x_val * inv_rms, inv_rms


def rms_back(normed, inv_rms, grad_norm):
    return inv_rms * (grad_norm - normed * jnp.mean(grad_norm * normed, axis=-1, keepdims=True))


def attend_seq(operands):
    q_seq, k_seq, v_seq, dout_seq, seq_len = operands
    q_grp = q_seq.reshape(SEQ, KV_SLOTS, GROUP, HEAD).astype(jnp.float32)
    k_full = k_seq.astype(jnp.float32)
    v_full = v_seq.astype(jnp.float32)
    dout_grp = dout_seq.reshape(SEQ, KV_SLOTS, GROUP, HEAD).astype(jnp.float32)
    row_pos = jnp.arange(SEQ)[:, None]
    col_pos = jnp.arange(SEQ)[None, :]
    visible = (col_pos <= row_pos) & (col_pos < seq_len)
    scores = jnp.einsum('igre,jge->grij', q_grp, k_full) * SCORE_SCALE
    scores = jnp.where(visible, scores, -1e30)
    attn_probs = jax.nn.softmax(scores, axis=-1)
    probs_b = attn_probs.astype(jnp.bfloat16).astype(jnp.float32)
    attn_out = jnp.einsum('grij,jge->igre', probs_b, v_full).astype(jnp.bfloat16)
    d_value = jnp.einsum('grij,igre->jge', probs_b, dout_grp).astype(jnp.bfloat16)
    d_probs = jnp.einsum('igre,jge->grij', dout_grp, v_full)
    d_scores = attn_probs * (d_probs - jnp.sum(d_probs * attn_probs, axis=-1, keepdims=True)) * SCORE_SCALE
    d_scores = d_scores.astype(jnp.bfloat16).astype(jnp.float32)
    d_query = jnp.einsum('grij,jge->igre', d_scores, k_full).astype(jnp.bfloat16)
    d_key = jnp.einsum('grij,igre->jge', d_scores, q_grp).astype(jnp.bfloat16)
    return attn_out.reshape(SEQ, HEADS, HEAD), d_query.reshape(SEQ, HEADS, HEAD), d_key, d_value


def layer_back(seq_lens, carry, layer_w):
    y_one, y_two, dy_one, dy_two = carry
    w_query, w_key, w_value, w_out, w_up, w_down = layer_w
    norm_g, inv_g = rms_norm(y_one.reshape(TOKENS, D))
    norm_g_b = norm_g.astype(jnp.bfloat16)
    pre_act = jnp.dot(norm_g_b, w_up, preferred_element_type=jnp.float32)
    act_val, gelu_back = jax.vjp(jax.nn.gelu, pre_act)
    act_b = act_val.astype(jnp.bfloat16)
    g_branch = jnp.dot(act_b, w_down, preferred_element_type=jnp.float32)
    x_two = y_two - g_branch.reshape(BATCH, SEQ, D)
    dy2_b = dy_two.reshape(TOKENS, D).astype(jnp.bfloat16)
    d_act = jnp.dot(dy2_b, w_down.T, preferred_element_type=jnp.float32)
    d_pre = gelu_back(d_act)[0].astype(jnp.bfloat16)
    dw_down = jnp.dot(act_b.T, dy2_b, preferred_element_type=jnp.float32)
    dw_up = jnp.dot(norm_g_b.T, d_pre, preferred_element_type=jnp.float32)
    grad_norm_g = jnp.dot(d_pre, w_up.T, preferred_element_type=jnp.float32)
    dy_one = dy_one + rms_back(norm_g, inv_g, grad_norm_g).reshape(BATCH, SEQ, D)

    norm_f, inv_f = rms_norm(x_two.reshape(TOKENS, D))
    norm_f_b = norm_f.astype(jnp.bfloat16)
    wq_flat = w_query.reshape(D, HEADS * HEAD)
    wk_flat = w_key.reshape(D, KV_SLOTS * HEAD)
    wv_flat = w_value.reshape(D, KV_SLOTS * HEAD)
    wo_flat = w_out.reshape(HEADS * HEAD, D)
    q_all = jnp.dot(norm_f_b, wq_flat, preferred_element_type=jnp.float32).astype(jnp.bfloat16).reshape(BATCH, SEQ, HEADS, HEAD)
    k_all = jnp.dot(norm_f_b, wk_flat, preferred_element_type=jnp.float32).astype(jnp.bfloat16).reshape(BATCH, SEQ, KV_SLOTS, HEAD)
    v_all = jnp.dot(norm_f_b, wv_flat, preferred_element_type=jnp.float32).astype(jnp.bfloat16).reshape(BATCH, SEQ, KV_SLOTS, HEAD)
    dy1_b = dy_one.reshape(TOKENS, D).astype(jnp.bfloat16)
    d_attn = jnp.dot(dy1_b, wo_flat.T, preferred_element_type=jnp.float32).astype(jnp.bfloat16).reshape(BATCH, SEQ, HEADS, HEAD)
    attn_out, d_query, d_key, d_value = lax.map(attend_seq, (q_all, k_all, v_all, d_attn, seq_lens))
    out_flat = attn_out.reshape(TOKENS, HEADS * HEAD)
    f_branch = jnp.dot(out_flat, wo_flat, preferred_element_type=jnp.float32)
    x_one = y_one - f_branch.reshape(BATCH, SEQ, D)
    dw_out = jnp.dot(out_flat.T, dy1_b, preferred_element_type=jnp.float32).reshape(HEADS, HEAD, D)
    dq_flat = d_query.reshape(TOKENS, HEADS * HEAD)
    dk_flat = d_key.reshape(TOKENS, KV_SLOTS * HEAD)
    dv_flat = d_value.reshape(TOKENS, KV_SLOTS * HEAD)
    dw_query = jnp.dot(norm_f_b.T, dq_flat, preferred_element_type=jnp.float32).reshape(D, HEADS, HEAD)
    dw_key = jnp.dot(norm_f_b.T, dk_flat, preferred_element_type=jnp.float32).reshape(D, KV_SLOTS, HEAD)
    dw_value = jnp.dot(norm_f_b.T, dv_flat, preferred_element_type=jnp.float32).reshape(D, KV_SLOTS, HEAD)
    grad_norm_f = (jnp.dot(dq_flat, wq_flat.T, preferred_element_type=jnp.float32)
                   + jnp.dot(dk_flat, wk_flat.T, preferred_element_type=jnp.float32)
                   + jnp.dot(dv_flat, wv_flat.T, preferred_element_type=jnp.float32))
    dx_two = dy_two + rms_back(norm_f, inv_f, grad_norm_f).reshape(BATCH, SEQ, D)
    return (x_one, x_two, dy_one, dx_two), (dw_query, dw_key, dw_value, dw_out, dw_up, dw_down)


def reference(y_one, y_two, dy_one, dy_two, seq_lens, w_query, w_key, w_value, w_out, w_up, w_down):
    end_state, layer_grads = lax.scan(functools.partial(layer_back, seq_lens), (y_one, y_two, dy_one, dy_two), (w_query, w_key, w_value, w_out, w_up, w_down), reverse=True)
    return (end_state[0], end_state[1], end_state[2], end_state[3], layer_grads[0], layer_grads[1], layer_grads[2], layer_grads[3], layer_grads[4], layer_grads[5])
```

```python
import functools
import jax
import jax.numpy as jnp
from jax import lax
from jax.experimental import pallas as pl
from jax.experimental.pallas import tpu as pltpu
from jax.sharding import PartitionSpec as P

F32 = jnp.float32
BF16 = jnp.bfloat16
EPS = 1e-5
MASK_VALUE = -1e30
MESH = pl.DeviceIdType.MESH
GELU_C = 0.7978845608028654
GELU_A = 0.044715

G, B, FW, DW = 0, 1, 2, 3
NT = (((1,), (1,)), ((), ()))
TN = (((0,), (0,)), ((), ()))


def dot_nn(a, b):
    return jnp.dot(a, b, preferred_element_type=F32)


def dot_nt(a, b):
    return lax.dot_general(a, b, NT, preferred_element_type=F32)


def dot_tn(a, b):
    return lax.dot_general(a, b, TN, preferred_element_type=F32)


def inv_rms(x_val):
    return lax.rsqrt(jnp.mean(x_val * x_val, axis=-1, keepdims=True) + EPS)


def rms_back(x_val, grad_norm):
    r = inv_rms(x_val)
    normed = x_val * r
    return r * (grad_norm - normed * jnp.mean(grad_norm * normed, axis=-1, keepdims=True))


def chain_kernel(lens_ref, y1_ref, y2_ref, d1_ref, d2_ref, wup_ref, wdn_ref, wq_ref, wk_ref, wv_ref, wo_ref,
                 on1, oh, ou, oe, on2, oa, oc, odqkv, ofin,
                 w1, w2, wa, wo, n1b, eb, n2b, cb, hb, ub, ab, dqb, gp, qkv, pbuf,
                 part, rd, sx, rx, st,
                 s_in, s_w, s_out, s_ds, s_dr, s_xs, s_xr, s_as, s_ar, s_fin,
                 *, n_layers, seq, d_model, ff, nq, nkv, head_dim, n_chunk):
    tokens = 4 * seq
    cw = d_model // n_chunk
    fw = ff // n_chunk
    me = lax.axis_index("tp")
    xi = lax.div(me, 2)
    ci = lax.rem(me, 2)
    xo = 1 - xi
    co = 1 - ci
    x_dev = {"tp": 2 * xo + ci}
    c_dev = {"tp": 2 * xi + co}
    score_scale = head_dim ** -0.5

    def rows(slot):
        return pl.ds(pl.multiple_of(slot * seq, seq), seq)

    def w_copies(lay, group):
        if group == 0:
            return [pltpu.make_async_copy(wup_ref.at[lay], w1, s_w.at[0])]
        if group == 1:
            return [pltpu.make_async_copy(wdn_ref.at[lay], w2, s_w.at[1])]
        if group == 2:
            return [pltpu.make_async_copy(wq_ref.at[lay], wa.at[pl.ds(0, nq)], s_w.at[2]),
                    pltpu.make_async_copy(wk_ref.at[lay], wa.at[pl.ds(nq, nkv)], s_w.at[4]),
                    pltpu.make_async_copy(wv_ref.at[lay], wa.at[pl.ds(nq + nkv, nkv)], s_w.at[5])]
        return [pltpu.make_async_copy(wo_ref.at[lay], wo, s_w.at[3])]

    def w_start(lay, group):
        for cp in w_copies(lay, group):
            cp.start()

    def w_wait(lay, group):
        for cp in w_copies(lay, group):
            cp.wait()

    def cols(k):
        return pl.ds(k * cw, cw)

    def d_copy(ty, k):
        return pltpu.make_async_remote_copy(
            part.at[ty, :, co, :, cols(k)], rd.at[ty, :, :, cols(k)], s_ds.at[ty, k], s_dr.at[ty, k],
            device_id=c_dev, device_id_type=MESH)

    def x_copy(ty, k):
        return pltpu.make_async_remote_copy(
            sx.at[ty, :, cols(k)], rx.at[ty, :, cols(k)], s_xs.at[ty, k], s_xr.at[ty, k],
            device_id=x_dev, device_id_type=MESH)

    def put_part(ty, k, val):
        part[ty, :, :, :, cols(k)] = val.reshape(2, 2, seq, cw)
        d_copy(ty, k).start()

    def mid(ty, k):
        d_copy(ty, k).wait_recv()
        sx[ty, :, cols(k)] = part[ty, xo, ci, :, cols(k)] + rd[ty, xo, :, cols(k)]
        x_copy(ty, k).start()

    def fin_sum(ty):
        for k in range(n_chunk):
            x_copy(ty, k).wait_recv()
        total = part[ty, xi, ci] + rd[ty, xi] + rx[ty]
        for k in range(n_chunk):
            x_copy(ty, k).wait_send()
            d_copy(ty, k).wait_send()
        return total

    ag_buf = {G: n2b, B: cb, FW: n1b, DW: eb}

    def ag_copy(ty, lay, step):
        buf = ag_buf[ty]
        slot = 2 * xo + ci if step == 2 else me
        return pltpu.make_async_remote_copy(
            buf.at[lay, rows(slot)], buf.at[lay, rows(slot)], s_as.at[ty, step], s_ar.at[ty, step],
            device_id=x_dev if step == 0 else c_dev, device_id_type=MESH)

    def ag_start(ty, lay, val):
        ag_buf[ty][lay, rows(me)] = val
        ag_copy(ty, lay, 0).start()
        ag_copy(ty, lay, 1).start()

    def ag_forward(ty, lay):
        ag_copy(ty, lay, 0).wait_recv()
        ag_copy(ty, lay, 2).start()

    def ag_ready(ty, lay):
        ag_copy(ty, lay, 1).wait_recv()
        ag_copy(ty, lay, 2).wait_recv()
        for step in range(3):
            ag_copy(ty, lay, step).wait_send()

    outs = [(on1, n1b), (oh, hb), (ou, ub), (oe, eb), (on2, n2b), (oa, ab), (oc, cb), (odqkv, dqb)]

    def out_copy(idx, lay):
        dst, src = outs[idx]
        return pltpu.make_async_copy(src.at[lay], dst.at[lay], s_out.at[idx, lay])

    def g_up(lay):
        for k in range(n_chunk):
            pre = dot_nn(n1b[lay], w1[:, pl.ds(k * fw, fw)])
            sq = pre * pre
            th = jnp.tanh(GELU_C * (pre + GELU_A * (sq * pre)))
            cdf = 0.5 * (1.0 + th)
            hb[lay, :, pl.ds(k * fw, fw)] = (pre * cdf).astype(BF16)
            gp[:, pl.ds(k * fw, fw)] = cdf + pre * (0.5 * (1.0 - th * th)) * (GELU_C * (1.0 + (3.0 * GELU_A) * sq))

    def g_down(lay):
        for k in range(n_chunk):
            put_part(G, k, dot_nn(hb[lay], w2[:, cols(k)]))
            if k >= 1:
                mid(G, k - 1)

    def b_up(lay):
        for k in range(n_chunk):
            d_act = dot_nt(eb[lay], w2[pl.ds(k * fw, fw), :])
            ub[lay, :, pl.ds(k * fw, fw)] = (gp[:, pl.ds(k * fw, fw)] * d_act).astype(BF16)

    def b_down(lay):
        for k in range(n_chunk):
            put_part(B, k, dot_nt(ub[lay], w1[cols(k), :]))

    lane = lax.broadcasted_iota(jnp.int32, (tokens, 2 * head_dim), 1)
    left = lane < head_dim

    def halves(blk):
        blk = blk.astype(F32)
        rolled = pltpu.roll(blk, head_dim, 1)
        zero = jnp.zeros_like(blk)
        return (((jnp.where(left, blk, zero)).astype(BF16), (jnp.where(left, zero, rolled)).astype(BF16)),
                ((jnp.where(left, rolled, zero)).astype(BF16), (jnp.where(left, zero, blk)).astype(BF16)))

    def visible():
        row = lax.broadcasted_iota(jnp.int32, (tokens, tokens), 0)
        col = lax.broadcasted_iota(jnp.int32, (tokens, tokens), 1)
        row_seq = lax.div(row, seq)
        limit = jnp.zeros((tokens, tokens), jnp.int32)
        for s in range(4):
            limit = jnp.where(row_seq == s, s * seq + lens_ref[s], limit)
        return (col <= row) & (col >= row_seq * seq) & (col < limit)

    n_pairs = nq // (2 * head_dim)
    pairs_per_slot = n_pairs // 2

    def f_fwd(lay):
        qkv[...] = dot_nt(n2b[lay], wa[...]).astype(BF16)
        keys = halves(qkv[:, nq:nq + nkv])
        vals = halves(qkv[:, nq + nkv:])
        vis = visible()
        for j in range(n_pairs):
            slot = j // pairs_per_slot
            q_pair = qkv[:, j * 2 * head_dim:(j + 1) * 2 * head_dim]
            att = None
            for half in range(2):
                s_val = jnp.where(vis, dot_nt(q_pair, keys[slot][half]) * score_scale, MASK_VALUE)
                ex = jnp.exp(s_val - jnp.max(s_val, axis=-1, keepdims=True))
                prob = ex / jnp.sum(ex, axis=-1, keepdims=True)
                pbuf[2 * j + half] = prob
                term = dot_nn(prob.astype(BF16), vals[slot][half])
                att = term if att is None else att + term
            ab[lay, :, j * 2 * head_dim:(j + 1) * 2 * head_dim] = att.astype(BF16)

    def f_out(lay):
        for k in range(n_chunk):
            put_part(FW, k, dot_nn(ab[lay], wo[:, cols(k)]))
            if k >= 1:
                mid(FW, k - 1)

    def d_attn(lay):
        d_out = dot_nt(cb[lay], wo[...]).astype(BF16)
        keys = halves(qkv[:, nq:nq + nkv])
        vals = halves(qkv[:, nq + nkv:])
        acc_v = [[None, None], [None, None]]
        acc_k = [[None, None], [None, None]]
        for j in range(n_pairs):
            slot = j // pairs_per_slot
            sl = slice(j * 2 * head_dim, (j + 1) * 2 * head_dim)
            q_pair = qkv[:, sl]
            d_pair = d_out[:, sl]
            dq = None
            for half in range(2):
                prob = pbuf[2 * j + half]
                tv = dot_tn(prob.astype(BF16), d_pair)
                dp = dot_nt(d_pair, vals[slot][half])
                row_dot = jnp.sum(prob * dp, axis=-1, keepdims=True)
                ds = (prob * (dp - row_dot) * score_scale).astype(BF16)
                tk = dot_tn(ds, q_pair)
                tq = dot_nn(ds, keys[slot][half])
                dq = tq if dq is None else dq + tq
                prev = acc_v[slot][half]
                acc_v[slot][half] = tv if prev is None else prev + tv
                prev = acc_k[slot][half]
                acc_k[slot][half] = tk if prev is None else prev + tk
            dqb[lay, :, sl] = dq.astype(BF16)

        def merge(acc):
            slot0 = acc[0][0] + pltpu.roll(acc[0][1], head_dim, 1)
            slot1 = pltpu.roll(acc[1][0], head_dim, 1) + acc[1][1]
            return jnp.where(left, slot0, slot1).astype(BF16)

        dqb[lay, :, nq:nq + nkv] = merge(acc_k)
        dqb[lay, :, nq + nkv:] = merge(acc_v)

    def d_out_step(lay):
        for k in range(n_chunk):
            put_part(DW, k, dot_nn(dqb[lay], wa[:, cols(k)]))

    def g_fin(lay):
        x2 = st[1] - fin_sum(G)
        st[1] = x2
        ag_start(G, lay, (x2 * inv_rms(x2)).astype(BF16))

    def b_fin(lay):
        dy1 = st[2] + rms_back(st[0], fin_sum(B))
        st[2] = dy1
        ag_start(B, lay, dy1.astype(BF16))

    def f_fin(lay, more):
        x1 = st[0] - fin_sum(FW)
        st[0] = x1

        @pl.when(more)
        def _():
            ag_start(FW, lay - 1, (x1 * inv_rms(x1)).astype(BF16))

    def d_fin(lay, more):
        dx2 = st[3] + rms_back(st[1], fin_sum(DW))
        st[3] = dx2

        @pl.when(more)
        def _():
            ag_start(DW, lay - 1, dx2.astype(BF16))

    top = n_layers - 1
    in_full = [pltpu.make_async_copy(y1_ref, part.at[FW], s_in.at[0]),
               pltpu.make_async_copy(d2_ref, part.at[DW], s_in.at[1])]
    in_own = [pltpu.make_async_copy(src.at[xi, ci], st.at[i], s_in.at[2 + i])
              for i, src in enumerate((y1_ref, y2_ref, d1_ref, d2_ref))]
    in_full[0].start()
    w_start(top, 0)
    in_full[1].start()
    w_start(top, 1)
    for cp in in_own:
        cp.start()
    w_start(top, 2)
    w_start(top, 3)
    barrier = pltpu.get_barrier_semaphore()
    pl.semaphore_signal(barrier, inc=1, device_id=x_dev, device_id_type=MESH)
    pl.semaphore_signal(barrier, inc=1, device_id=c_dev, device_id_type=MESH)
    in_full[0].wait()
    for a in range(2):
        for b in range(2):
            y_val = part[FW, a, b]
            n1b[top, pl.ds((2 * a + b) * seq, seq)] = (y_val * inv_rms(y_val)).astype(BF16)
    in_full[1].wait()
    for a in range(2):
        for b in range(2):
            eb[top, pl.ds((2 * a + b) * seq, seq)] = part[DW, a, b].astype(BF16)
    for cp in in_own:
        cp.wait()
    pl.semaphore_wait(barrier, 2)

    def layer_body(i, carry):
        lay = top - i
        more = i < top
        not_first = i > 0
        w_wait(lay, 0)
        g_up(lay)
        out_copy(0, lay).start()
        out_copy(1, lay).start()
        w_wait(lay, 1)
        g_down(lay)

        @pl.when(not_first)
        def _():
            d_fin(lay + 1, True)

        mid(G, n_chunk - 1)

        @pl.when(not_first)
        def _():
            ag_forward(DW, lay)
            ag_ready(DW, lay)

        b_up(lay)
        b_down(lay)
        out_copy(2, lay).start()
        out_copy(3, lay).start()

        @pl.when(more)
        def _():
            w_start(lay - 1, 0)
            w_start(lay - 1, 1)

        g_fin(lay)
        for k in range(n_chunk):
            mid(B, k)
        ag_forward(G, lay)
        ag_ready(G, lay)
        out_copy(4, lay).start()
        w_wait(lay, 2)
        f_fwd(lay)
        w_wait(lay, 3)
        f_out(lay)
        out_copy(5, lay).start()
        mid(FW, n_chunk - 1)
        b_fin(lay)
        ag_forward(B, lay)
        ag_ready(B, lay)
        out_copy(6, lay).start()
        d_attn(lay)
        d_out_step(lay)
        out_copy(7, lay).start()

        @pl.when(more)
        def _():
            w_start(lay - 1, 2)
            w_start(lay - 1, 3)

        f_fin(lay, more)
        for k in range(n_chunk):
            mid(DW, k)

        @pl.when(more)
        def _():
            ag_forward(FW, lay - 1)
            ag_ready(FW, lay - 1)

        return carry

    lax.fori_loop(0, n_layers, layer_body, 0)
    d_fin(0, False)
    fin = pltpu.make_async_copy(st, ofin, s_fin)
    fin.start()
    for idx in range(8):
        for lay in range(n_layers):
            out_copy(idx, lay).wait()
    fin.wait()


def run_chain(lens, y1, y2, d1, d2, w_up, w_down, wq, wk, wv, wo):
    n_layers, d_model, ff = w_up.shape
    seq = y1.shape[2]
    tokens = 4 * seq
    nq, nkv = wq.shape[1], wk.shape[1]
    head_dim = nkv // 2
    n_chunk = 4
    n_w = nq + 2 * nkv
    body = functools.partial(chain_kernel, n_layers=n_layers, seq=seq, d_model=d_model, ff=ff, nq=nq, nkv=nkv,
                             head_dim=head_dim, n_chunk=n_chunk)
    any_spec = pl.BlockSpec(memory_space=pl.ANY)
    wide = jax.ShapeDtypeStruct((n_layers, tokens, d_model), BF16)
    wide_ff = jax.ShapeDtypeStruct((n_layers, tokens, ff), BF16)
    out_shape = [wide, wide_ff, wide_ff, wide, wide, jax.ShapeDtypeStruct((n_layers, tokens, nq), BF16), wide,
                 jax.ShapeDtypeStruct((n_layers, tokens, n_w), BF16),
                 jax.ShapeDtypeStruct((4, seq, d_model), F32)]
    vm = pltpu.VMEM
    dma = pltpu.SemaphoreType.DMA
    scratch = [vm((d_model, ff), BF16), vm((ff, d_model), BF16), vm((n_w, d_model), BF16), vm((nq, d_model), BF16),
               vm((n_layers, tokens, d_model), BF16), vm((n_layers, tokens, d_model), BF16),
               vm((n_layers, tokens, d_model), BF16), vm((n_layers, tokens, d_model), BF16),
               vm((n_layers, tokens, ff), BF16), vm((n_layers, tokens, ff), BF16),
               vm((n_layers, tokens, nq), BF16), vm((n_layers, tokens, n_w), BF16),
               vm((tokens, ff), F32), vm((tokens, n_w), BF16), vm((nq // head_dim, tokens, tokens), F32),
               vm((4, 2, 2, seq, d_model), F32), vm((4, 2, seq, d_model), F32),
               vm((4, seq, d_model), F32), vm((4, seq, d_model), F32), vm((4, seq, d_model), F32),
               dma((6,)), dma((6,)), dma((8, n_layers)),
               dma((4, n_chunk)), dma((4, n_chunk)), dma((4, n_chunk)), dma((4, n_chunk)),
               dma((4, 3)), dma((4, 3)), dma]
    return pl.pallas_call(
        body, out_shape=out_shape,
        in_specs=[pl.BlockSpec(memory_space=pltpu.SMEM)] + [any_spec] * 10,
        out_specs=[any_spec] * 9,
        scratch_shapes=scratch,
        compiler_params=pltpu.CompilerParams(collective_id=0, has_side_effects=True, vmem_limit_bytes=60 * 2 ** 20),
        cost_estimate=pl.CostEstimate(flops=60 * 10 ** 9, bytes_accessed=10 ** 8, transcendentals=0),
        name="chain",
    )(lens, y1, y2, d1, d2, w_up, w_down, wq, wk, wv, wo)


def ff_grad_kernel(n1_ref, u_ref, h_ref, e_ref, dup_ref, ddn_ref):
    dup_ref[0] = dot_tn(n1_ref[0], u_ref[0])
    ddn_ref[0] = dot_tn(h_ref[0], e_ref[0])


def ff_grads(n1, u, h, e):
    n_layers, tokens, d_model = n1.shape
    ff = u.shape[2]
    n_tiles = 8
    rd, rf = d_model // n_tiles, ff // n_tiles
    return pl.pallas_call(
        ff_grad_kernel, grid=(n_layers, n_tiles),
        out_shape=[jax.ShapeDtypeStruct((n_layers, d_model, ff), F32), jax.ShapeDtypeStruct((n_layers, ff, d_model), F32)],
        in_specs=[pl.BlockSpec((1, tokens, rd), lambda l, t: (l, 0, t)), pl.BlockSpec((1, tokens, ff), lambda l, t: (l, 0, 0)),
                  pl.BlockSpec((1, tokens, rf), lambda l, t: (l, 0, t)), pl.BlockSpec((1, tokens, d_model), lambda l, t: (l, 0, 0))],
        out_specs=[pl.BlockSpec((1, rd, ff), lambda l, t: (l, t, 0)), pl.BlockSpec((1, rf, d_model), lambda l, t: (l, t, 0))],
        compiler_params=pltpu.CompilerParams(dimension_semantics=("arbitrary", "arbitrary")),
        cost_estimate=pl.CostEstimate(flops=30 * 10 ** 9, bytes_accessed=10 ** 8, transcendentals=0),
        name="ff_grads",
    )(n1, u, h, e)


def attn_grad_kernel(dqkv_ref, n2_ref, a_ref, c_ref, dq_ref, dk_ref, dv_ref, do_ref, *, nq, nkv):
    n2 = n2_ref[0]
    dq_ref[0] = dot_tn(dqkv_ref[0, :, :nq], n2)
    dk_ref[0] = dot_tn(dqkv_ref[0, :, nq:nq + nkv], n2)
    dv_ref[0] = dot_tn(dqkv_ref[0, :, nq + nkv:], n2)
    do_ref[0] = dot_tn(a_ref[0], c_ref[0])


def attn_grads(dqkv, n2, a, c, nq, nkv):
    n_layers, tokens, d_model = n2.shape
    n_tiles = 2
    cw = d_model // n_tiles
    n_w = nq + 2 * nkv
    return pl.pallas_call(
        functools.partial(attn_grad_kernel, nq=nq, nkv=nkv), grid=(n_layers, n_tiles),
        out_shape=[jax.ShapeDtypeStruct((n_layers, r, d_model), F32) for r in (nq, nkv, nkv, nq)],
        in_specs=[pl.BlockSpec((1, tokens, n_w), lambda l, t: (l, 0, 0)), pl.BlockSpec((1, tokens, cw), lambda l, t: (l, 0, t)),
                  pl.BlockSpec((1, tokens, nq), lambda l, t: (l, 0, 0)), pl.BlockSpec((1, tokens, cw), lambda l, t: (l, 0, t))],
        out_specs=[pl.BlockSpec((1, r, cw), lambda l, t: (l, 0, t)) for r in (nq, nkv, nkv, nq)],
        compiler_params=pltpu.CompilerParams(dimension_semantics=("arbitrary", "arbitrary")),
        cost_estimate=pl.CostEstimate(flops=10 * 10 ** 9, bytes_accessed=3 * 10 ** 7, transcendentals=0),
        name="attn_grads",
    )(dqkv, n2, a, c)


def gather_tp(own):
    me = lax.axis_index("tp")
    across = lax.ppermute(own, "tp", [(0, 2), (2, 0), (1, 3), (3, 1)])
    chip = jnp.stack([own, across])
    other = lax.ppermute(chip, "tp", [(0, 1), (1, 0), (2, 3), (3, 2)])
    own_chip = jnp.where(me < 2, chip, chip[::-1])
    oth_chip = jnp.where(me < 2, other, other[::-1])
    even = lax.rem(me, 2) == 0
    first = jnp.where(even, own_chip, oth_chip)
    second = jnp.where(even, oth_chip, own_chip)
    return [jnp.stack([first[0, i], second[0, i], first[1, i], second[1, i]]) for i in range(4)]


def solution(mesh):
    act_spec = P('dp', None, None)
    w_specs = (P(None, None, 'tp', None), P(None, None, 'tp', None), P(None, None, 'tp', None),
               P(None, 'tp', None, None), P(None, None, 'tp'), P(None, 'tp', None))
    g_specs = (P('dp', None, 'tp', None), P('dp', None, 'tp', None), P('dp', None, 'tp', None),
               P('dp', 'tp', None, None), P('dp', None, 'tp'), P('dp', 'tp', None))

    def local_fn(y_one, y_two, dy_one, dy_two, seq_lens, w_query, w_key, w_value, w_out, w_up, w_down):
        n_layers, d_model, heads, head_dim = w_query.shape
        slots = w_key.shape[2]
        seq = y_one.shape[1]
        nq, nkv = heads * head_dim, slots * head_dim

        def to_rows(w, width):
            return jnp.transpose(w, (0, 2, 3, 1)).reshape(n_layers, width, d_model)

        def from_rows(g, n_heads):
            return jnp.transpose(g.reshape(n_layers, n_heads, head_dim, d_model), (0, 3, 1, 2))

        acts = [a.reshape(2, 2, seq, d_model) for a in (y_one, y_two, dy_one, dy_two)]
        n1, h, u, e, n2, a, c, dqkv, fin = run_chain(
            seq_lens, *acts, w_up, w_down, to_rows(w_query, nq), to_rows(w_key, nkv), to_rows(w_value, nkv),
            w_out.reshape(n_layers, nq, d_model))
        gathered = gather_tp(fin)
        d_up, d_down = ff_grads(n1, u, h, e)
        dq, dk, dv, do = attn_grads(dqkv, n2, a, c, nq, nkv)
        outs = gathered
        return (outs[0], outs[1], outs[2], outs[3],
                from_rows(dq, heads), from_rows(dk, slots), from_rows(dv, slots),
                do.reshape(n_layers, heads, head_dim, d_model), d_up, d_down)

    return jax.shard_map(local_fn, mesh=mesh,
                         in_specs=(act_spec,) * 4 + (P('dp'),) + w_specs,
                         out_specs=(act_spec,) * 4 + g_specs,
                         check_vma=False)
```

```python
import functools
import jax
import jax.numpy as jnp
from jax import lax
from jax.experimental import pallas as pl
from jax.experimental.pallas import tpu as pltpu
from jax.sharding import PartitionSpec as P

F32 = jnp.float32
BF16 = jnp.bfloat16
EPS = 1e-5
MASK_VALUE = -1e30
MESH = pl.DeviceIdType.MESH
GELU_C = 0.7978845608028654
GELU_A = 0.044715

G, B, FW, DW = 0, 1, 2, 3
NT = (((1,), (1,)), ((), ()))
TN = (((0,), (0,)), ((), ()))


def dot_nn(a, b):
    return jnp.dot(a, b, preferred_element_type=F32)


def dot_nt(a, b):
    return lax.dot_general(a, b, NT, preferred_element_type=F32)


def dot_tn(a, b):
    return lax.dot_general(a, b, TN, preferred_element_type=F32)


def inv_rms(x_val):
    return lax.rsqrt(jnp.mean(x_val * x_val, axis=-1, keepdims=True) + EPS)


def rms_back(x_val, grad_norm):
    r = inv_rms(x_val)
    normed = x_val * r
    return r * (grad_norm - normed * jnp.mean(grad_norm * normed, axis=-1, keepdims=True))


def chain_kernel(lens_ref, y1_ref, y2_ref, d1_ref, d2_ref, wup_ref, wdn_ref, wq_ref, wk_ref, wv_ref, wo_ref,
                 on1, oh, ou, oe, on2, oa, oc, odqkv, ofin,
                 w1, w2, wa, wo, n1b, eb, n2b, cb, hb, ub, ab, dqb, gp, qkv, pbuf,
                 part, rd, sx, rx, st,
                 s_in, s_w, s_out, s_ds, s_dr, s_xs, s_xr, s_as, s_ar, s_fin,
                 *, n_layers, seq, d_model, ff, nq, nkv, head_dim, n_chunk):
    tokens = 4 * seq
    cw = d_model // n_chunk
    fw = ff // n_chunk
    me = lax.axis_index("tp")
    xi = lax.div(me, 2)
    ci = lax.rem(me, 2)
    xo = 1 - xi
    co = 1 - ci
    x_dev = {"tp": 2 * xo + ci}
    c_dev = {"tp": 2 * xi + co}
    score_scale = head_dim ** -0.5

    def rows(slot):
        return pl.ds(pl.multiple_of(slot * seq, seq), seq)

    W_ATT = 2 * n_chunk
    W_OUT = W_ATT + 1

    def cols(k):
        return pl.ds(k * cw, cw)

    def w_copies(lay, group):
        if group < n_chunk:
            sl = pl.ds(group * fw, fw)
            return [pltpu.make_async_copy(wup_ref.at[lay, :, sl], w1.at[:, sl], s_w.at[group])]
        if group < 2 * n_chunk:
            return [pltpu.make_async_copy(wdn_ref.at[lay, :, cols(group - n_chunk)], w2.at[:, cols(group - n_chunk)],
                                          s_w.at[group])]
        if group == W_ATT:
            return [pltpu.make_async_copy(wq_ref.at[lay], wa.at[pl.ds(0, nq)], s_w.at[group]),
                    pltpu.make_async_copy(wk_ref.at[lay], wa.at[pl.ds(nq, nkv)], s_w.at[group + 2]),
                    pltpu.make_async_copy(wv_ref.at[lay], wa.at[pl.ds(nq + nkv, nkv)], s_w.at[group + 3])]
        return [pltpu.make_async_copy(wo_ref.at[lay], wo, s_w.at[group])]

    def w_start(lay, group):
        for cp in w_copies(lay, group):
            cp.start()

    def w_wait(lay, group):
        for cp in w_copies(lay, group):
            cp.wait()

    def d_copy(ty, k):
        return pltpu.make_async_remote_copy(
            part.at[ty, :, co, :, cols(k)], rd.at[ty, :, :, cols(k)], s_ds.at[ty, k], s_dr.at[ty, k],
            device_id=c_dev, device_id_type=MESH)

    def x_copy(ty, k):
        return pltpu.make_async_remote_copy(
            sx.at[ty, :, cols(k)], rx.at[ty, :, cols(k)], s_xs.at[ty, k], s_xr.at[ty, k],
            device_id=x_dev, device_id_type=MESH)

    def put_part(ty, k, val):
        part[ty, :, :, :, cols(k)] = val.reshape(2, 2, seq, cw)
        d_copy(ty, k).start()

    def mid(ty, k):
        d_copy(ty, k).wait_recv()
        sx[ty, :, cols(k)] = part[ty, xo, ci, :, cols(k)] + rd[ty, xo, :, cols(k)]
        x_copy(ty, k).start()

    def fin_sum(ty):
        for k in range(n_chunk):
            x_copy(ty, k).wait_recv()
        total = part[ty, xi, ci] + rd[ty, xi] + rx[ty]
        for k in range(n_chunk):
            x_copy(ty, k).wait_send()
            d_copy(ty, k).wait_send()
        return total

    ag_buf = {G: n2b, B: cb, FW: n1b, DW: eb}

    def ag_copy(ty, lay, step):
        buf = ag_buf[ty]
        slot = 2 * xo + ci if step == 2 else me
        return pltpu.make_async_remote_copy(
            buf.at[lay, rows(slot)], buf.at[lay, rows(slot)], s_as.at[ty, step], s_ar.at[ty, step],
            device_id=x_dev if step == 0 else c_dev, device_id_type=MESH)

    def ag_start(ty, lay, val):
        ag_buf[ty][lay, rows(me)] = val
        ag_copy(ty, lay, 0).start()
        ag_copy(ty, lay, 1).start()

    def ag_forward(ty, lay):
        ag_copy(ty, lay, 0).wait_recv()
        ag_copy(ty, lay, 2).start()

    def ag_ready(ty, lay):
        ag_copy(ty, lay, 1).wait_recv()
        ag_copy(ty, lay, 2).wait_recv()
        for step in range(3):
            ag_copy(ty, lay, step).wait_send()

    outs = [(on1, n1b), (oh, hb), (ou, ub), (oe, eb), (on2, n2b), (oa, ab), (oc, cb), (odqkv, dqb)]

    def out_copy(idx, lay):
        dst, src = outs[idx]
        return pltpu.make_async_copy(src.at[lay], dst.at[lay], s_out.at[idx, lay])

    def g_up(lay):
        for k in range(n_chunk):
            w_wait(lay, k)
            pre = dot_nn(n1b[lay], w1[:, pl.ds(k * fw, fw)])
            sq = pre * pre
            th = jnp.tanh(GELU_C * (pre + GELU_A * (sq * pre)))
            cdf = 0.5 * (1.0 + th)
            hb[lay, :, pl.ds(k * fw, fw)] = (pre * cdf).astype(BF16)
            gp[:, pl.ds(k * fw, fw)] = cdf + pre * (0.5 * (1.0 - th * th)) * (GELU_C * (1.0 + (3.0 * GELU_A) * sq))

    def g_put(lay, k):
        w_wait(lay, n_chunk + k)
        put_part(G, k, dot_nn(hb[lay], w2[:, cols(k)]))

    def b_up(lay, k):
        d_act = dot_nt(eb[lay], w2[pl.ds(k * fw, fw), :])
        ub[lay, :, pl.ds(k * fw, fw)] = (gp[:, pl.ds(k * fw, fw)] * d_act).astype(BF16)

    def b_put(lay, k):
        put_part(B, k, dot_nt(ub[lay], w1[cols(k), :]))

    lane = lax.broadcasted_iota(jnp.int32, (tokens, 2 * head_dim), 1)
    left = lane < head_dim

    def halves(blk):
        blk = blk.astype(F32)
        rolled = pltpu.roll(blk, head_dim, 1)
        zero = jnp.zeros_like(blk)
        return (((jnp.where(left, blk, zero)).astype(BF16), (jnp.where(left, zero, rolled)).astype(BF16)),
                ((jnp.where(left, rolled, zero)).astype(BF16), (jnp.where(left, zero, blk)).astype(BF16)))

    def visible():
        row = lax.broadcasted_iota(jnp.int32, (tokens, tokens), 0)
        col = lax.broadcasted_iota(jnp.int32, (tokens, tokens), 1)
        row_seq = lax.div(row, seq)
        limit = jnp.zeros((tokens, tokens), jnp.int32)
        for s in range(4):
            limit = jnp.where(row_seq == s, s * seq + lens_ref[s], limit)
        return (col <= row) & (col >= row_seq * seq) & (col < limit)

    n_pairs = nq // (2 * head_dim)
    pairs_per_slot = n_pairs // 2

    def f_proj(lay):
        qkv[...] = dot_nt(n2b[lay], wa[...]).astype(BF16)

    def f_attn(lay):
        keys = halves(qkv[:, nq:nq + nkv])
        vals = halves(qkv[:, nq + nkv:])
        vis = visible()
        for j in range(n_pairs):
            slot = j // pairs_per_slot
            q_pair = qkv[:, j * 2 * head_dim:(j + 1) * 2 * head_dim]
            att = None
            for half in range(2):
                s_val = jnp.where(vis, dot_nt(q_pair, keys[slot][half]) * score_scale, MASK_VALUE)
                ex = jnp.exp(s_val - jnp.max(s_val, axis=-1, keepdims=True))
                prob = ex / jnp.sum(ex, axis=-1, keepdims=True)
                pbuf[2 * j + half] = prob
                term = dot_nn(prob.astype(BF16), vals[slot][half])
                att = term if att is None else att + term
            ab[lay, :, j * 2 * head_dim:(j + 1) * 2 * head_dim] = att.astype(BF16)

    def f_put(lay, k):
        put_part(FW, k, dot_nn(ab[lay], wo[:, cols(k)]))

    def d_attn(lay):
        d_out = dot_nt(cb[lay], wo[...]).astype(BF16)
        keys = halves(qkv[:, nq:nq + nkv])
        vals = halves(qkv[:, nq + nkv:])
        acc_v = [[None, None], [None, None]]
        acc_k = [[None, None], [None, None]]
        for j in range(n_pairs):
            slot = j // pairs_per_slot
            sl = slice(j * 2 * head_dim, (j + 1) * 2 * head_dim)
            q_pair = qkv[:, sl]
            d_pair = d_out[:, sl]
            dq = None
            for half in range(2):
                prob = pbuf[2 * j + half]
                tv = dot_tn(prob.astype(BF16), d_pair)
                dp = dot_nt(d_pair, vals[slot][half])
                row_dot = jnp.sum(prob * dp, axis=-1, keepdims=True)
                ds = (prob * (dp - row_dot) * score_scale).astype(BF16)
                tk = dot_tn(ds, q_pair)
                tq = dot_nn(ds, keys[slot][half])
                dq = tq if dq is None else dq + tq
                prev = acc_v[slot][half]
                acc_v[slot][half] = tv if prev is None else prev + tv
                prev = acc_k[slot][half]
                acc_k[slot][half] = tk if prev is None else prev + tk
            dqb[lay, :, sl] = dq.astype(BF16)

        def merge(acc):
            slot0 = acc[0][0] + pltpu.roll(acc[0][1], head_dim, 1)
            slot1 = pltpu.roll(acc[1][0], head_dim, 1) + acc[1][1]
            return jnp.where(left, slot0, slot1).astype(BF16)

        dqb[lay, :, nq:nq + nkv] = merge(acc_k)
        dqb[lay, :, nq + nkv:] = merge(acc_v)

    def d_put(lay, k):
        put_part(DW, k, dot_nn(dqb[lay], wa[:, cols(k)]))

    def g_fin(lay):
        x2 = st[1] - fin_sum(G)
        st[1] = x2
        ag_start(G, lay, (x2 * inv_rms(x2)).astype(BF16))

    def b_fin(lay):
        dy1 = st[2] + rms_back(st[0], fin_sum(B))
        st[2] = dy1
        ag_start(B, lay, dy1.astype(BF16))

    def f_fin(lay, more):
        x1 = st[0] - fin_sum(FW)
        st[0] = x1
        if more:
            ag_start(FW, lay - 1, (x1 * inv_rms(x1)).astype(BF16))

    def d_fin(lay, more):
        dx2 = st[3] + rms_back(st[1], fin_sum(DW))
        st[3] = dx2
        if more:
            ag_start(DW, lay - 1, dx2.astype(BF16))

    top = n_layers - 1
    in_full = [pltpu.make_async_copy(y1_ref, part.at[FW], s_in.at[0]),
               pltpu.make_async_copy(d2_ref, part.at[DW], s_in.at[1])]
    in_own = [pltpu.make_async_copy(src.at[xi, ci], st.at[i], s_in.at[2 + i])
              for i, src in enumerate((y1_ref, y2_ref, d1_ref, d2_ref))]
    in_full[0].start()
    for k in range(2 * n_chunk):
        w_start(top, k)
    in_full[1].start()
    for cp in in_own:
        cp.start()
    w_start(top, W_ATT)
    w_start(top, W_OUT)
    barrier = pltpu.get_barrier_semaphore()
    pl.semaphore_signal(barrier, inc=1, device_id=x_dev, device_id_type=MESH)
    pl.semaphore_signal(barrier, inc=1, device_id=c_dev, device_id_type=MESH)
    in_full[0].wait()
    for a in range(2):
        for b in range(2):
            y_val = part[FW, a, b]
            n1b[top, pl.ds((2 * a + b) * seq, seq)] = (y_val * inv_rms(y_val)).astype(BF16)
    pl.semaphore_wait(barrier, 2)

    def layer_body(i, carry):
        lay = top - i
        more = i < top
        first = i == 0
        later = i > 0

        @pl.when(later)
        def _():
            f_fin(lay + 1, True)
            d_fin(lay + 1, True)
            ag_forward(FW, lay)
            ag_ready(FW, lay)

        g_up(lay)
        out_copy(0, lay).start()
        out_copy(1, lay).start()
        g_put(lay, 0)

        @pl.when(later)
        def _():
            ag_forward(DW, lay)

        g_put(lay, 1)
        g_put(lay, 2)
        mid(G, 0)
        g_put(lay, 3)
        mid(G, 1)

        @pl.when(later)
        def _():
            ag_ready(DW, lay)

        @pl.when(first)
        def _():
            in_full[1].wait()
            for a in range(2):
                for b in range(2):
                    eb[top, pl.ds((2 * a + b) * seq, seq)] = part[DW, a, b].astype(BF16)
            for cp in in_own:
                cp.wait()

        b_up(lay, 0)
        mid(G, 2)
        mid(G, 3)
        for k in range(1, n_chunk):
            b_up(lay, k)
        out_copy(2, lay).start()
        out_copy(3, lay).start()
        b_put(lay, 0)
        b_put(lay, 1)
        mid(B, 0)
        b_put(lay, 2)
        b_put(lay, 3)

        @pl.when(more)
        def _():
            for k in range(2 * n_chunk):
                w_start(lay - 1, k)

        mid(B, 1)
        mid(B, 2)
        g_fin(lay)
        mid(B, 3)
        ag_forward(G, lay)
        b_fin(lay)
        ag_ready(G, lay)
        out_copy(4, lay).start()
        w_wait(lay, W_ATT)
        f_proj(lay)
        f_attn(lay)
        out_copy(5, lay).start()
        w_wait(lay, W_OUT)
        f_put(lay, 0)
        f_put(lay, 1)
        f_put(lay, 2)
        f_put(lay, 3)
        mid(FW, 0)
        mid(FW, 1)
        ag_forward(B, lay)
        mid(FW, 2)
        mid(FW, 3)
        ag_ready(B, lay)
        out_copy(6, lay).start()
        d_attn(lay)
        out_copy(7, lay).start()
        for k in range(n_chunk):
            d_put(lay, k)

        @pl.when(more)
        def _():
            w_start(lay - 1, W_ATT)
            w_start(lay - 1, W_OUT)

        for k in range(n_chunk):
            mid(DW, k)
        return carry

    lax.fori_loop(0, n_layers, layer_body, 0)
    f_fin(0, False)
    d_fin(0, False)
    fin = pltpu.make_async_copy(st, ofin, s_fin)
    fin.start()
    for idx in range(8):
        for lay in range(n_layers):
            out_copy(idx, lay).wait()
    fin.wait()


def run_chain(lens, y1, y2, d1, d2, w_up, w_down, wq, wk, wv, wo):
    n_layers, d_model, ff = w_up.shape
    seq = y1.shape[2]
    tokens = 4 * seq
    nq, nkv = wq.shape[1], wk.shape[1]
    head_dim = nkv // 2
    n_chunk = 4
    n_w = nq + 2 * nkv
    body = functools.partial(chain_kernel, n_layers=n_layers, seq=seq, d_model=d_model, ff=ff, nq=nq, nkv=nkv,
                             head_dim=head_dim, n_chunk=n_chunk)
    any_spec = pl.BlockSpec(memory_space=pl.ANY)
    wide = jax.ShapeDtypeStruct((n_layers, tokens, d_model), BF16)
    wide_ff = jax.ShapeDtypeStruct((n_layers, tokens, ff), BF16)
    out_shape = [wide, wide_ff, wide_ff, wide, wide, jax.ShapeDtypeStruct((n_layers, tokens, nq), BF16), wide,
                 jax.ShapeDtypeStruct((n_layers, tokens, n_w), BF16),
                 jax.ShapeDtypeStruct((4, seq, d_model), F32)]
    vm = pltpu.VMEM
    dma = pltpu.SemaphoreType.DMA
    scratch = [vm((d_model, ff), BF16), vm((ff, d_model), BF16), vm((n_w, d_model), BF16), vm((nq, d_model), BF16),
               vm((n_layers, tokens, d_model), BF16), vm((n_layers, tokens, d_model), BF16),
               vm((n_layers, tokens, d_model), BF16), vm((n_layers, tokens, d_model), BF16),
               vm((n_layers, tokens, ff), BF16), vm((n_layers, tokens, ff), BF16),
               vm((n_layers, tokens, nq), BF16), vm((n_layers, tokens, n_w), BF16),
               vm((tokens, ff), F32), vm((tokens, n_w), BF16), vm((nq // head_dim, tokens, tokens), F32),
               vm((4, 2, 2, seq, d_model), F32), vm((4, 2, seq, d_model), F32),
               vm((4, seq, d_model), F32), vm((4, seq, d_model), F32), vm((4, seq, d_model), F32),
               dma((6,)), dma((2 * n_chunk + 4,)), dma((8, n_layers)),
               dma((4, n_chunk)), dma((4, n_chunk)), dma((4, n_chunk)), dma((4, n_chunk)),
               dma((4, 3)), dma((4, 3)), dma]
    return pl.pallas_call(
        body, out_shape=out_shape,
        in_specs=[pl.BlockSpec(memory_space=pltpu.SMEM)] + [any_spec] * 10,
        out_specs=[any_spec] * 9,
        scratch_shapes=scratch,
        compiler_params=pltpu.CompilerParams(collective_id=0, has_side_effects=True, vmem_limit_bytes=60 * 2 ** 20),
        cost_estimate=pl.CostEstimate(flops=60 * 10 ** 9, bytes_accessed=10 ** 8, transcendentals=0),
        name="chain",
    )(lens, y1, y2, d1, d2, w_up, w_down, wq, wk, wv, wo)


def grad_kernel(*refs, nq, nkv, n_tiles, start, n_prev, has_acts):
    n1_ref, u_ref, h_ref, e_ref, dqkv_ref, n2_ref, a_ref, c_ref = refs[:8]
    pos = 8
    if has_acts:
        srcs = refs[pos:pos + 4]
        pos += 4
    pos += n_prev
    dup_ref, ddn_ref, dq_ref, dk_ref, dv_ref, do_ref = refs[pos:pos + 6]
    pos += 6
    idx = pl.program_id(0)
    step = lax.rem(idx + start, n_tiles)
    dup_ref[0] = dot_tn(n1_ref[0], u_ref[0])
    ddn_ref[0] = dot_tn(h_ref[0], e_ref[0])
    tile = pl.ds(pl.multiple_of(lax.div(step, 2) * 128, 128), 128)

    @pl.when(lax.rem(step, 2) == 0)
    def _():
        dq_ref[0] = dot_tn(dqkv_ref[0, :, tile], n2_ref[0])

    @pl.when(lax.rem(step, 2) == 1)
    def _():
        do_ref[0] = dot_tn(a_ref[0, :, tile], c_ref[0])

    @pl.when((step == 1) | (idx == 0))
    def _():
        dk_ref[0] = dot_tn(dqkv_ref[0, :, nq:nq + nkv], n2_ref[0])

    @pl.when((step == 2) | (idx == 0))
    def _():
        dv_ref[0] = dot_tn(dqkv_ref[0, :, nq + nkv:], n2_ref[0])

    if has_acts:
        out_refs = refs[pos:pos + 4]
        buf, s_ld, s_st = refs[pos + 4:]
        me = lax.axis_index("tp")
        xi, ci = lax.div(me, 2), lax.rem(me, 2)
        slots = (me, 2 * (1 - xi) + ci, 2 * xi + 1 - ci, 2 * (1 - xi) + 1 - ci)

        def load(i):
            return pltpu.make_async_copy(srcs[i], buf.at[i], s_ld.at[i])

        def store(i, j):
            return pltpu.make_async_copy(buf.at[i, j], out_refs[j].at[slots[i]], s_st.at[i, j])

        @pl.when(idx == 0)
        def _():
            for i in range(4):
                load(i).start()

        @pl.when(idx == 2)
        def _():
            for i in range(4):
                load(i).wait()
                for j in range(4):
                    store(i, j).start()

        @pl.when(idx == 5)
        def _():
            for i in range(4):
                for j in range(4):
                    store(i, j).wait()


def weight_grads(ops, start, count, nq, nkv, prev=None, acts=None):
    n1, u, h, e, dqkv, n2, a, c = ops
    n_layers, tokens, d_model = n1.shape
    ff = u.shape[2]
    n_tiles = 2 * nq // 128
    rd, rf = d_model // n_tiles, ff // n_tiles
    n_w = nq + 2 * nkv

    def lay(i):
        return (i + start) // n_tiles

    def tile_of(i):
        return (i + start) % n_tiles

    def full(width):
        return pl.BlockSpec((1, tokens, width), lambda i: (lay(i), 0, 0))

    def tile(width):
        return pl.BlockSpec((1, tokens, width), lambda i: (lay(i), 0, tile_of(i)))

    def rows(n_rows, width):
        return pl.BlockSpec((1, n_rows, width), lambda i: (lay(i), tile_of(i), 0))

    def half(n_rows, width):
        return pl.BlockSpec((1, n_rows, width), lambda i: (lay(i), tile_of(i) // 2, 0))

    def whole(n_rows, width):
        return pl.BlockSpec((1, n_rows, width), lambda i: (lay(i), 0, 0))

    in_specs = [tile(rd), full(ff), tile(rf), full(d_model), full(n_w), full(d_model), full(nq), full(d_model)]
    operands = list(ops)
    any_spec = pl.BlockSpec(memory_space=pl.ANY)
    out_shape = [jax.ShapeDtypeStruct((n_layers, r, w), F32)
                 for r, w in ((d_model, ff), (ff, d_model), (nq, d_model), (nkv, d_model), (nkv, d_model), (nq, d_model))]
    out_specs = [rows(rd, ff), rows(rf, d_model), half(128, d_model), whole(nkv, d_model), whole(nkv, d_model),
                 half(128, d_model)]
    scratch = []
    if acts is not None:
        operands += list(acts)
        in_specs += [any_spec] * 4
    aliases = {}
    if prev is not None:
        aliases = {len(operands) + i: i for i in range(6)}
        operands += list(prev)
        in_specs += [any_spec] * 6
    if acts is not None:
        seq = acts[0].shape[1]
        out_shape += [jax.ShapeDtypeStruct((4, seq, d_model), F32)] * 4
        out_specs += [any_spec] * 4
        scratch = [pltpu.VMEM((4, 4, seq, d_model), F32), pltpu.SemaphoreType.DMA((4,)), pltpu.SemaphoreType.DMA((4, 4))]
    return pl.pallas_call(
        functools.partial(grad_kernel, nq=nq, nkv=nkv, n_tiles=n_tiles, start=start,
                          n_prev=6 if prev is not None else 0, has_acts=acts is not None),
        grid=(count,), out_shape=out_shape, in_specs=in_specs, out_specs=out_specs, scratch_shapes=scratch,
        input_output_aliases=aliases,
        compiler_params=pltpu.CompilerParams(dimension_semantics=("arbitrary",)),
        cost_estimate=pl.CostEstimate(flops=10 ** 9 * count, bytes_accessed=6 * 10 ** 6 * count, transcendentals=0),
        name="weight_grads",
    )(*operands)


def solution(mesh):
    act_spec = P('dp', None, None)
    w_specs = (P(None, None, 'tp', None), P(None, None, 'tp', None), P(None, None, 'tp', None),
               P(None, 'tp', None, None), P(None, None, 'tp'), P(None, 'tp', None))
    g_specs = (P('dp', None, 'tp', None), P('dp', None, 'tp', None), P('dp', None, 'tp', None),
               P('dp', 'tp', None, None), P('dp', None, 'tp'), P('dp', 'tp', None))

    def local_fn(y_one, y_two, dy_one, dy_two, seq_lens, w_query, w_key, w_value, w_out, w_up, w_down):
        n_layers, d_model, heads, head_dim = w_query.shape
        slots = w_key.shape[2]
        seq = y_one.shape[1]
        nq, nkv = heads * head_dim, slots * head_dim

        def to_rows(w, width):
            return jnp.transpose(w, (0, 2, 3, 1)).reshape(n_layers, width, d_model)

        def from_rows(g, n_heads):
            return jnp.transpose(g.reshape(n_layers, n_heads, head_dim, d_model), (0, 3, 1, 2))

        acts = [a.reshape(2, 2, seq, d_model) for a in (y_one, y_two, dy_one, dy_two)]
        n1, h, u, e, n2, a, c, dqkv, fin = run_chain(
            seq_lens, *acts, w_up, w_down, to_rows(w_query, nq), to_rows(w_key, nkv), to_rows(w_value, nkv),
            w_out.reshape(n_layers, nq, d_model))
        ops = (n1, u, h, e, dqkv, n2, a, c)
        across = lax.ppermute(fin, "tp", [(0, 2), (2, 0), (1, 3), (3, 1)])
        cores = [(0, 1), (1, 0), (2, 3), (3, 2)]
        near = lax.ppermute(fin, "tp", cores)
        n_steps = n_layers * (2 * nq // 128)
        cut_a = n_steps // 2
        cut_b = cut_a + 4
        grads = weight_grads(ops, 0, cut_a, nq, nkv)
        across, dk = lax.optimization_barrier((across, grads[3]))
        grads = list(grads[:3]) + [dk] + list(grads[4:])
        far = lax.ppermute(across, "tp", cores)
        grads = weight_grads(ops, cut_a, cut_b - cut_a, nq, nkv, prev=grads)
        res = weight_grads(ops, cut_b, n_steps - cut_b, nq, nkv, prev=grads, acts=(fin, across, near, far))
        d_up, d_down, dq, dk, dv, do = res[:6]
        outs = [o.reshape(y_one.shape) for o in res[6:]]
        return (outs[0], outs[1], outs[2], outs[3],
                from_rows(dq, heads), from_rows(dk, slots), from_rows(dv, slots),
                do.reshape(n_layers, heads, head_dim, d_model), d_up, d_down)

    return jax.shard_map(local_fn, mesh=mesh,
                         in_specs=(act_spec,) * 4 + (P('dp'),) + w_specs,
                         out_specs=(act_spec,) * 4 + g_specs,
                         check_vma=False)
```

```python
import functools
import jax
import jax.numpy as jnp
from jax import lax
from jax.experimental import pallas as pl
from jax.experimental.pallas import tpu as pltpu
from jax.sharding import PartitionSpec as P

F32 = jnp.float32
BF16 = jnp.bfloat16
EPS = 1e-5
MASK_VALUE = -1e30
MESH = pl.DeviceIdType.MESH
GELU_C = 0.7978845608028654
GELU_A = 0.044715

G, B, FW, DW = 0, 1, 2, 3
NT = (((1,), (1,)), ((), ()))
TN = (((0,), (0,)), ((), ()))


def dot_nn(a, b):
    return jnp.dot(a, b, preferred_element_type=F32)


def dot_nt(a, b):
    return lax.dot_general(a, b, NT, preferred_element_type=F32)


def dot_tn(a, b):
    return lax.dot_general(a, b, TN, preferred_element_type=F32)


def inv_rms(x_val):
    return lax.rsqrt(jnp.mean(x_val * x_val, axis=-1, keepdims=True) + EPS)


def rms_back(x_val, grad_norm):
    r = inv_rms(x_val)
    normed = x_val * r
    return r * (grad_norm - normed * jnp.mean(grad_norm * normed, axis=-1, keepdims=True))


def chain_kernel(lens_ref, y1_ref, y2_ref, d1_ref, d2_ref, wup_ref, wdn_ref, wq_ref, wk_ref, wv_ref, wo_ref,
                 on1, oh, ou, oe, on2, oa, oc, odqkv, o_early, o_base, o_send, o_own,
                 w1, w2, wa, wo, n1b, eb, n2b, cb, hb, ub, ab, dqb, gp, qkv, pbuf,
                 part, rd, sx, rx, st,
                 s_in, s_w, s_out, s_ds, s_dr, s_xs, s_xr, s_as, s_ar, s_fin,
                 *, n_layers, seq, d_model, ff, nq, nkv, head_dim, n_chunk):
    tokens = 4 * seq
    cw = d_model // n_chunk
    fw = ff // n_chunk
    me = lax.axis_index("tp")
    xi = lax.div(me, 2)
    ci = lax.rem(me, 2)
    xo = 1 - xi
    co = 1 - ci
    x_dev = {"tp": 2 * xo + ci}
    c_dev = {"tp": 2 * xi + co}
    score_scale = head_dim ** -0.5

    def rows(slot):
        return pl.ds(pl.multiple_of(slot * seq, seq), seq)

    W_ATT = 2 * n_chunk
    W_OUT = W_ATT + 1

    def cols(k):
        return pl.ds(k * cw, cw)

    def w_copies(lay, group):
        if group < n_chunk:
            sl = pl.ds(group * fw, fw)
            return [pltpu.make_async_copy(wup_ref.at[lay, :, sl], w1.at[:, sl], s_w.at[group])]
        if group < 2 * n_chunk:
            return [pltpu.make_async_copy(wdn_ref.at[lay, :, cols(group - n_chunk)], w2.at[:, cols(group - n_chunk)],
                                          s_w.at[group])]
        if group == W_ATT:
            return [pltpu.make_async_copy(wq_ref.at[lay], wa.at[pl.ds(0, nq)], s_w.at[group]),
                    pltpu.make_async_copy(wk_ref.at[lay], wa.at[pl.ds(nq, nkv)], s_w.at[group + 2]),
                    pltpu.make_async_copy(wv_ref.at[lay], wa.at[pl.ds(nq + nkv, nkv)], s_w.at[group + 3])]
        return [pltpu.make_async_copy(wo_ref.at[lay], wo, s_w.at[group])]

    def w_start(lay, group):
        for cp in w_copies(lay, group):
            cp.start()

    def w_wait(lay, group):
        for cp in w_copies(lay, group):
            cp.wait()

    def d_copy(ty, k):
        return pltpu.make_async_remote_copy(
            part.at[ty, :, co, :, cols(k)], rd.at[ty, :, :, cols(k)], s_ds.at[ty, k], s_dr.at[ty, k],
            device_id=c_dev, device_id_type=MESH)

    def x_copy(ty, k):
        return pltpu.make_async_remote_copy(
            sx.at[ty, :, cols(k)], rx.at[ty, :, cols(k)], s_xs.at[ty, k], s_xr.at[ty, k],
            device_id=x_dev, device_id_type=MESH)

    def put_part(ty, k, val):
        part[ty, :, :, :, cols(k)] = val.reshape(2, 2, seq, cw)
        d_copy(ty, k).start()

    def mid(ty, k, send=None):
        d_copy(ty, k).wait_recv()
        sx[ty, :, cols(k)] = part[ty, xo, ci, :, cols(k)] + rd[ty, xo, :, cols(k)]
        if send is None:
            x_copy(ty, k).start()
        else:
            @pl.when(send)
            def _():
                x_copy(ty, k).start()

    def fin_sum(ty):
        for k in range(n_chunk):
            x_copy(ty, k).wait_recv()
        total = part[ty, xi, ci] + rd[ty, xi] + rx[ty]
        for k in range(n_chunk):
            x_copy(ty, k).wait_send()
            d_copy(ty, k).wait_send()
        return total

    ag_buf = {G: n2b, B: cb, FW: n1b, DW: eb}

    def ag_copy(ty, lay, step):
        buf = ag_buf[ty]
        slot = 2 * xo + ci if step == 2 else me
        return pltpu.make_async_remote_copy(
            buf.at[lay, rows(slot)], buf.at[lay, rows(slot)], s_as.at[ty, step], s_ar.at[ty, step],
            device_id=x_dev if step == 0 else c_dev, device_id_type=MESH)

    def ag_start(ty, lay, val):
        ag_buf[ty][lay, rows(me)] = val
        ag_copy(ty, lay, 0).start()
        ag_copy(ty, lay, 1).start()

    def ag_forward(ty, lay):
        ag_copy(ty, lay, 0).wait_recv()
        ag_copy(ty, lay, 2).start()

    def ag_ready(ty, lay):
        ag_copy(ty, lay, 1).wait_recv()
        ag_copy(ty, lay, 2).wait_recv()
        for step in range(3):
            ag_copy(ty, lay, step).wait_send()

    outs = [(on1, n1b), (oh, hb), (ou, ub), (oe, eb), (on2, n2b), (oa, ab), (oc, cb), (odqkv, dqb)]

    def out_copy(idx, lay):
        dst, src = outs[idx]
        return pltpu.make_async_copy(src.at[lay], dst.at[lay], s_out.at[idx, lay])

    def g_up(lay):
        for k in range(n_chunk):
            w_wait(lay, k)
            pre = dot_nn(n1b[lay], w1[:, pl.ds(k * fw, fw)])
            sq = pre * pre
            th = jnp.tanh(GELU_C * (pre + GELU_A * (sq * pre)))
            cdf = 0.5 * (1.0 + th)
            hb[lay, :, pl.ds(k * fw, fw)] = (pre * cdf).astype(BF16)
            gp[:, pl.ds(k * fw, fw)] = cdf + pre * (0.5 * (1.0 - th * th)) * (GELU_C * (1.0 + (3.0 * GELU_A) * sq))

    def g_put(lay, k):
        w_wait(lay, n_chunk + k)
        put_part(G, k, dot_nn(hb[lay], w2[:, cols(k)]))

    def b_up(lay, k):
        d_act = dot_nt(eb[lay], w2[pl.ds(k * fw, fw), :])
        ub[lay, :, pl.ds(k * fw, fw)] = (gp[:, pl.ds(k * fw, fw)] * d_act).astype(BF16)

    def b_put(lay, k):
        put_part(B, k, dot_nt(ub[lay], w1[cols(k), :]))

    lane = lax.broadcasted_iota(jnp.int32, (tokens, 2 * head_dim), 1)
    left = lane < head_dim

    def halves(blk):
        blk = blk.astype(F32)
        rolled = pltpu.roll(blk, head_dim, 1)
        zero = jnp.zeros_like(blk)
        return (((jnp.where(left, blk, zero)).astype(BF16), (jnp.where(left, zero, rolled)).astype(BF16)),
                ((jnp.where(left, rolled, zero)).astype(BF16), (jnp.where(left, zero, blk)).astype(BF16)))

    def visible():
        row = lax.broadcasted_iota(jnp.int32, (tokens, tokens), 0)
        col = lax.broadcasted_iota(jnp.int32, (tokens, tokens), 1)
        row_seq = lax.div(row, seq)
        limit = jnp.zeros((tokens, tokens), jnp.int32)
        for s in range(4):
            limit = jnp.where(row_seq == s, s * seq + lens_ref[s], limit)
        return (col <= row) & (col >= row_seq * seq) & (col < limit)

    n_pairs = nq // (2 * head_dim)
    pairs_per_slot = n_pairs // 2

    def f_proj(lay):
        qkv[...] = dot_nt(n2b[lay], wa[...]).astype(BF16)

    def f_attn(lay):
        keys = halves(qkv[:, nq:nq + nkv])
        vals = halves(qkv[:, nq + nkv:])
        vis = visible()
        for j in range(n_pairs):
            slot = j // pairs_per_slot
            q_pair = qkv[:, j * 2 * head_dim:(j + 1) * 2 * head_dim]
            att = None
            for half in range(2):
                s_val = jnp.where(vis, dot_nt(q_pair, keys[slot][half]) * score_scale, MASK_VALUE)
                ex = jnp.exp(s_val - jnp.max(s_val, axis=-1, keepdims=True))
                prob = ex / jnp.sum(ex, axis=-1, keepdims=True)
                pbuf[2 * j + half] = prob
                term = dot_nn(prob.astype(BF16), vals[slot][half])
                att = term if att is None else att + term
            ab[lay, :, j * 2 * head_dim:(j + 1) * 2 * head_dim] = att.astype(BF16)

    def f_put(lay, k):
        put_part(FW, k, dot_nn(ab[lay], wo[:, cols(k)]))

    def d_attn(lay):
        d_out = dot_nt(cb[lay], wo[...]).astype(BF16)
        keys = halves(qkv[:, nq:nq + nkv])
        vals = halves(qkv[:, nq + nkv:])
        acc_v = [[None, None], [None, None]]
        acc_k = [[None, None], [None, None]]
        for j in range(n_pairs):
            slot = j // pairs_per_slot
            sl = slice(j * 2 * head_dim, (j + 1) * 2 * head_dim)
            q_pair = qkv[:, sl]
            d_pair = d_out[:, sl]
            dq = None
            for half in range(2):
                prob = pbuf[2 * j + half]
                tv = dot_tn(prob.astype(BF16), d_pair)
                dp = dot_nt(d_pair, vals[slot][half])
                row_dot = jnp.sum(prob * dp, axis=-1, keepdims=True)
                ds = (prob * (dp - row_dot) * score_scale).astype(BF16)
                tk = dot_tn(ds, q_pair)
                tq = dot_nn(ds, keys[slot][half])
                dq = tq if dq is None else dq + tq
                prev = acc_v[slot][half]
                acc_v[slot][half] = tv if prev is None else prev + tv
                prev = acc_k[slot][half]
                acc_k[slot][half] = tk if prev is None else prev + tk
            dqb[lay, :, sl] = dq.astype(BF16)

        def merge(acc):
            slot0 = acc[0][0] + pltpu.roll(acc[0][1], head_dim, 1)
            slot1 = pltpu.roll(acc[1][0], head_dim, 1) + acc[1][1]
            return jnp.where(left, slot0, slot1).astype(BF16)

        dqb[lay, :, nq:nq + nkv] = merge(acc_k)
        dqb[lay, :, nq + nkv:] = merge(acc_v)

    def d_put(lay, k):
        put_part(DW, k, dot_nn(dqb[lay], wa[:, cols(k)]))

    def g_fin(lay):
        x2 = st[2] - fin_sum(G)
        st[2] = x2
        ag_start(G, lay, (x2 * inv_rms(x2)).astype(BF16))

    def b_fin(lay):
        dy1 = st[3] + rms_back(st[0], fin_sum(B))
        st[3] = dy1
        ag_start(B, lay, dy1.astype(BF16))

    def f_fin(lay):
        x1 = st[0] - fin_sum(FW)
        st[0] = x1
        ag_start(FW, lay - 1, (x1 * inv_rms(x1)).astype(BF16))

    def d_fin(lay):
        dx2 = st[1] + rms_back(st[2], fin_sum(DW))
        st[1] = dx2
        ag_start(DW, lay - 1, dx2.astype(BF16))

    top = n_layers - 1
    in_full = [pltpu.make_async_copy(y1_ref, part.at[FW], s_in.at[0]),
               pltpu.make_async_copy(d2_ref, part.at[DW], s_in.at[1])]
    in_own = [pltpu.make_async_copy(src.at[xi, ci], st.at[i], s_in.at[2 + i])
              for i, src in enumerate((y1_ref, d2_ref, y2_ref, d1_ref))]
    in_full[0].start()
    for k in range(2 * n_chunk):
        w_start(top, k)
    in_full[1].start()
    for cp in in_own:
        cp.start()
    w_start(top, W_ATT)
    w_start(top, W_OUT)
    barrier = pltpu.get_barrier_semaphore()
    pl.semaphore_signal(barrier, inc=1, device_id=x_dev, device_id_type=MESH)
    pl.semaphore_signal(barrier, inc=1, device_id=c_dev, device_id_type=MESH)
    in_full[0].wait()
    for a in range(2):
        for b in range(2):
            y_val = part[FW, a, b]
            n1b[top, pl.ds((2 * a + b) * seq, seq)] = (y_val * inv_rms(y_val)).astype(BF16)
    pl.semaphore_wait(barrier, 2)

    def layer_body(i, carry):
        lay = top - i
        more = i < top
        first = i == 0
        later = i > 0

        @pl.when(later)
        def _():
            f_fin(lay + 1)
            d_fin(lay + 1)
            ag_forward(FW, lay)
            ag_ready(FW, lay)

        g_up(lay)
        out_copy(0, lay).start()
        out_copy(1, lay).start()
        g_put(lay, 0)

        @pl.when(later)
        def _():
            ag_forward(DW, lay)

        g_put(lay, 1)
        g_put(lay, 2)
        mid(G, 0)
        g_put(lay, 3)
        mid(G, 1)

        @pl.when(later)
        def _():
            ag_ready(DW, lay)

        @pl.when(first)
        def _():
            in_full[1].wait()
            for a in range(2):
                for b in range(2):
                    eb[top, pl.ds((2 * a + b) * seq, seq)] = part[DW, a, b].astype(BF16)
            for cp in in_own:
                cp.wait()

        b_up(lay, 0)
        mid(G, 2)
        mid(G, 3)
        for k in range(1, n_chunk):
            b_up(lay, k)
        out_copy(2, lay).start()
        out_copy(3, lay).start()
        b_put(lay, 0)
        b_put(lay, 1)
        mid(B, 0)
        b_put(lay, 2)
        b_put(lay, 3)

        @pl.when(more)
        def _():
            for k in range(2 * n_chunk):
                w_start(lay - 1, k)

        mid(B, 1)
        mid(B, 2)
        g_fin(lay)
        mid(B, 3)
        ag_forward(G, lay)
        b_fin(lay)
        ag_ready(G, lay)
        out_copy(4, lay).start()
        w_wait(lay, W_ATT)
        f_proj(lay)
        f_attn(lay)
        out_copy(5, lay).start()
        w_wait(lay, W_OUT)
        f_put(lay, 0)
        f_put(lay, 1)
        f_put(lay, 2)
        f_put(lay, 3)
        mid(FW, 0, more)
        mid(FW, 1, more)
        ag_forward(B, lay)
        mid(FW, 2, more)
        mid(FW, 3, more)
        ag_ready(B, lay)
        out_copy(6, lay).start()
        d_attn(lay)
        out_copy(7, lay).start()
        for k in range(n_chunk):
            d_put(lay, k)

        @pl.when(more)
        def _():
            w_start(lay - 1, W_ATT)
            w_start(lay - 1, W_OUT)

        for k in range(n_chunk):
            mid(DW, k, more)
        return carry

    lax.fori_loop(0, n_layers, layer_body, 0)
    for ty in (FW, DW):
        rx[ty] = part[ty, xi, ci] + rd[ty, xi]
    tail = [pltpu.make_async_copy(src, dst, s_fin.at[i]) for i, (src, dst) in enumerate(
        ((st.at[pl.ds(2, 2)], o_early), (st.at[pl.ds(0, 2)], o_base),
         (sx.at[pl.ds(FW, 2)], o_send), (rx.at[pl.ds(FW, 2)], o_own)))]
    for cp in tail:
        cp.start()
    for ty in (FW, DW):
        for k in range(n_chunk):
            d_copy(ty, k).wait_send()
    for idx in range(8):
        for lay in range(n_layers):
            out_copy(idx, lay).wait()
    for cp in tail:
        cp.wait()


def run_chain(lens, y1, y2, d1, d2, w_up, w_down, wq, wk, wv, wo):
    n_layers, d_model, ff = w_up.shape
    seq = y1.shape[2]
    tokens = 4 * seq
    nq, nkv = wq.shape[1], wk.shape[1]
    head_dim = nkv // 2
    n_chunk = 4
    n_w = nq + 2 * nkv
    body = functools.partial(chain_kernel, n_layers=n_layers, seq=seq, d_model=d_model, ff=ff, nq=nq, nkv=nkv,
                             head_dim=head_dim, n_chunk=n_chunk)
    any_spec = pl.BlockSpec(memory_space=pl.ANY)
    wide = jax.ShapeDtypeStruct((n_layers, tokens, d_model), BF16)
    wide_ff = jax.ShapeDtypeStruct((n_layers, tokens, ff), BF16)
    out_shape = [wide, wide_ff, wide_ff, wide, wide, jax.ShapeDtypeStruct((n_layers, tokens, nq), BF16), wide,
                 jax.ShapeDtypeStruct((n_layers, tokens, n_w), BF16),
                 ] + [jax.ShapeDtypeStruct((2, seq, d_model), F32)] * 4
    vm = pltpu.VMEM
    dma = pltpu.SemaphoreType.DMA
    scratch = [vm((d_model, ff), BF16), vm((ff, d_model), BF16), vm((n_w, d_model), BF16), vm((nq, d_model), BF16),
               vm((n_layers, tokens, d_model), BF16), vm((n_layers, tokens, d_model), BF16),
               vm((n_layers, tokens, d_model), BF16), vm((n_layers, tokens, d_model), BF16),
               vm((n_layers, tokens, ff), BF16), vm((n_layers, tokens, ff), BF16),
               vm((n_layers, tokens, nq), BF16), vm((n_layers, tokens, n_w), BF16),
               vm((tokens, ff), F32), vm((tokens, n_w), BF16), vm((nq // head_dim, tokens, tokens), F32),
               vm((4, 2, 2, seq, d_model), F32), vm((4, 2, seq, d_model), F32),
               vm((4, seq, d_model), F32), vm((4, seq, d_model), F32), vm((4, seq, d_model), F32),
               dma((6,)), dma((2 * n_chunk + 4,)), dma((8, n_layers)),
               dma((4, n_chunk)), dma((4, n_chunk)), dma((4, n_chunk)), dma((4, n_chunk)),
               dma((4, 3)), dma((4, 3)), dma((4,))]
    return pl.pallas_call(
        body, out_shape=out_shape,
        in_specs=[pl.BlockSpec(memory_space=pltpu.SMEM)] + [any_spec] * 10,
        out_specs=[any_spec] * 12,
        scratch_shapes=scratch,
        compiler_params=pltpu.CompilerParams(collective_id=0, has_side_effects=True, vmem_limit_bytes=60 * 2 ** 20),
        cost_estimate=pl.CostEstimate(flops=60 * 10 ** 9, bytes_accessed=10 ** 8, transcendentals=0),
        name="chain",
    )(lens, y1, y2, d1, d2, w_up, w_down, wq, wk, wv, wo)


def grad_kernel(*refs, nq, nkv, n_tiles, start, n_prev):
    n1_ref, u_ref, h_ref, e_ref, dqkv_ref, n2_ref, a_ref, c_ref = refs[:8]
    pos = 8 + n_prev
    dup_ref, ddn_ref, dq_ref, dk_ref, dv_ref, do_ref = refs[pos:pos + 6]
    idx = pl.program_id(0)
    step = lax.rem(idx + start, n_tiles)
    dup_ref[0] = dot_tn(n1_ref[0], u_ref[0])
    ddn_ref[0] = dot_tn(h_ref[0], e_ref[0])
    tile = pl.ds(pl.multiple_of(lax.div(step, 2) * 128, 128), 128)

    @pl.when(lax.rem(step, 2) == 0)
    def _():
        dq_ref[0] = dot_tn(dqkv_ref[0, :, tile], n2_ref[0])

    @pl.when(lax.rem(step, 2) == 1)
    def _():
        do_ref[0] = dot_tn(a_ref[0, :, tile], c_ref[0])

    @pl.when((step == 1) | (idx == 0))
    def _():
        dk_ref[0] = dot_tn(dqkv_ref[0, :, nq:nq + nkv], n2_ref[0])

    @pl.when((step == 2) | (idx == 0))
    def _():
        dv_ref[0] = dot_tn(dqkv_ref[0, :, nq + nkv:], n2_ref[0])


def weight_grads(ops, start, count, nq, nkv, prev=None):
    n1, u, h, e, dqkv, n2, a, c = ops
    n_layers, tokens, d_model = n1.shape
    ff = u.shape[2]
    n_tiles = 2 * nq // 128
    rd, rf = d_model // n_tiles, ff // n_tiles
    n_w = nq + 2 * nkv

    def lay(i):
        return (i + start) // n_tiles

    def tile_of(i):
        return (i + start) % n_tiles

    def full(width):
        return pl.BlockSpec((1, tokens, width), lambda i: (lay(i), 0, 0))

    def tile(width):
        return pl.BlockSpec((1, tokens, width), lambda i: (lay(i), 0, tile_of(i)))

    def rows(n_rows, width):
        return pl.BlockSpec((1, n_rows, width), lambda i: (lay(i), tile_of(i), 0))

    def half(n_rows, width):
        return pl.BlockSpec((1, n_rows, width), lambda i: (lay(i), tile_of(i) // 2, 0))

    def whole(n_rows, width):
        return pl.BlockSpec((1, n_rows, width), lambda i: (lay(i), 0, 0))

    in_specs = [tile(rd), full(ff), tile(rf), full(d_model), full(n_w), full(d_model), full(nq), full(d_model)]
    operands = list(ops)
    any_spec = pl.BlockSpec(memory_space=pl.ANY)
    out_shape = [jax.ShapeDtypeStruct((n_layers, r, w), F32)
                 for r, w in ((d_model, ff), (ff, d_model), (nq, d_model), (nkv, d_model), (nkv, d_model), (nq, d_model))]
    out_specs = [rows(rd, ff), rows(rf, d_model), half(128, d_model), whole(nkv, d_model), whole(nkv, d_model),
                 half(128, d_model)]
    aliases = {}
    if prev is not None:
        aliases = {len(operands) + i: i for i in range(6)}
        operands += list(prev)
        in_specs += [any_spec] * 6
    return pl.pallas_call(
        functools.partial(grad_kernel, nq=nq, nkv=nkv, n_tiles=n_tiles, start=start,
                          n_prev=6 if prev is not None else 0),
        grid=(count,), out_shape=out_shape, in_specs=in_specs, out_specs=out_specs,
        input_output_aliases=aliases,
        compiler_params=pltpu.CompilerParams(dimension_semantics=("arbitrary",)),
        cost_estimate=pl.CostEstimate(flops=10 ** 9 * count, bytes_accessed=6 * 10 ** 6 * count, transcendentals=0),
        name="weight_grads",
    )(*operands)


def last_kernel(base_ref, early_ref, own_ref, got_ref, late_ref):
    late_ref[0] = base_ref[0] - (own_ref[0] + got_ref[0])
    late_ref[1] = base_ref[1] + rms_back(early_ref[0], own_ref[1] + got_ref[1])


def last_sums(base, early, own, got):
    vmem = pl.BlockSpec(memory_space=pltpu.VMEM)
    return pl.pallas_call(
        last_kernel, out_shape=jax.ShapeDtypeStruct(base.shape, F32), in_specs=[vmem] * 4, out_specs=vmem,
        compiler_params=pltpu.CompilerParams(vmem_limit_bytes=8 * 2 ** 20), name="last_sums",
    )(base, early, own, got)


def place_kernel(*refs):
    early, late, out_refs, sems = refs[:4], refs[4:8], refs[8:12], refs[12]
    me = lax.axis_index("tp")
    xi, ci = lax.div(me, 2), lax.rem(me, 2)
    slots = (me, 2 * (1 - xi) + ci, 2 * xi + 1 - ci, 2 * (1 - xi) + 1 - ci)
    copies = []
    for i in range(4):
        for j, src in enumerate((late[i].at[0], early[i].at[0], early[i].at[1], late[i].at[1])):
            copies.append(pltpu.make_async_copy(src, out_refs[j].at[slots[i]], sems.at[i, j]))
    for cp in copies:
        cp.start()
    for cp in copies:
        cp.wait()


def place(early, late):
    _, seq, d_model = early[0].shape
    return pl.pallas_call(
        place_kernel, out_shape=[jax.ShapeDtypeStruct((4, seq, d_model), F32)] * 4,
        in_specs=[pl.BlockSpec(memory_space=pltpu.VMEM)] * 8, out_specs=[pl.BlockSpec(memory_space=pl.ANY)] * 4,
        scratch_shapes=[pltpu.SemaphoreType.DMA((4, 4))],
        compiler_params=pltpu.CompilerParams(vmem_limit_bytes=16 * 2 ** 20), name="place",
    )(*early, *late)


def solution(mesh):
    act_spec = P('dp', None, None)
    w_specs = (P(None, None, 'tp', None), P(None, None, 'tp', None), P(None, None, 'tp', None),
               P(None, 'tp', None, None), P(None, None, 'tp'), P(None, 'tp', None))
    g_specs = (P('dp', None, 'tp', None), P('dp', None, 'tp', None), P('dp', None, 'tp', None),
               P('dp', 'tp', None, None), P('dp', None, 'tp'), P('dp', 'tp', None))

    def local_fn(y_one, y_two, dy_one, dy_two, seq_lens, w_query, w_key, w_value, w_out, w_up, w_down):
        n_layers, d_model, heads, head_dim = w_query.shape
        slots = w_key.shape[2]
        seq = y_one.shape[1]
        nq, nkv = heads * head_dim, slots * head_dim

        def to_rows(w, width):
            return jnp.transpose(w, (0, 2, 3, 1)).reshape(n_layers, width, d_model)

        def from_rows(g, n_heads):
            return jnp.transpose(g.reshape(n_layers, n_heads, head_dim, d_model), (0, 3, 1, 2))

        acts = [a.reshape(2, 2, seq, d_model) for a in (y_one, y_two, dy_one, dy_two)]
        n1, h, u, e, n2, a, c, dqkv, early, base, send, own = run_chain(
            seq_lens, *acts, w_up, w_down, to_rows(w_query, nq), to_rows(w_key, nkv), to_rows(w_value, nkv),
            w_out.reshape(n_layers, nq, d_model))
        ops = (n1, u, h, e, dqkv, n2, a, c)
        chips = [(0, 2), (2, 0), (1, 3), (3, 1)]
        cores = [(0, 1), (1, 0), (2, 3), (3, 2)]
        got = lax.ppermute(send, "tp", chips)
        early_c = lax.ppermute(early, "tp", cores)
        n_steps = n_layers * (2 * nq // 128)
        cut = n_steps // 4

        def tie(grads, *vals):
            tied = lax.optimization_barrier((grads[3],) + vals)
            return list(grads[:3]) + [tied[0]] + list(grads[4:]), tied[1:]

        grads = weight_grads(ops, 0, cut, nq, nkv)
        grads, (got, early) = tie(grads, got, early)
        late = last_sums(base, early, own, got)
        grads, (late,) = tie(grads, late)
        late_x = lax.ppermute(late, "tp", chips)
        early_x = lax.ppermute(early, "tp", chips)
        late_c = lax.ppermute(late, "tp", cores)
        grads = weight_grads(ops, cut, n_steps - cut, nq, nkv, prev=grads)
        grads, (early_x, late_x) = tie(grads, early_x, late_x)
        early_d = lax.ppermute(early_x, "tp", cores)
        late_d = lax.ppermute(late_x, "tp", cores)
        d_up, d_down, dq, dk, dv, do = grads
        outs = [o.reshape(y_one.shape) for o in place((early, early_x, early_c, early_d), (late, late_x, late_c, late_d))]
        return (outs[0], outs[1], outs[2], outs[3],
                from_rows(dq, heads), from_rows(dk, slots), from_rows(dv, slots),
                do.reshape(n_layers, heads, head_dim, d_model), d_up, d_down)

    return jax.shard_map(local_fn, mesh=mesh,
                         in_specs=(act_spec,) * 4 + (P('dp'),) + w_specs,
                         out_specs=(act_spec,) * 4 + g_specs,
                         check_vma=False)
```

```python
import functools
import jax
import jax.numpy as jnp
from jax import lax
from jax.experimental import pallas as pl
from jax.experimental.pallas import tpu as pltpu
from jax.sharding import PartitionSpec as P

F32 = jnp.float32
BF16 = jnp.bfloat16
EPS = 1e-5
MASK_VALUE = -1e30
MESH = pl.DeviceIdType.MESH
GELU_C = 0.7978845608028654
GELU_A = 0.044715

G, B, FW, DW = 0, 1, 2, 3
NT = (((1,), (1,)), ((), ()))
TN = (((0,), (0,)), ((), ()))


def dot_nn(a, b):
    return jnp.dot(a, b, preferred_element_type=F32)


def dot_nt(a, b):
    return lax.dot_general(a, b, NT, preferred_element_type=F32)


def dot_tn(a, b):
    return lax.dot_general(a, b, TN, preferred_element_type=F32)


def inv_rms(x_val):
    return lax.rsqrt(jnp.mean(x_val * x_val, axis=-1, keepdims=True) + EPS)


def rms_back(x_val, grad_norm):
    r = inv_rms(x_val)
    normed = x_val * r
    return r * (grad_norm - normed * jnp.mean(grad_norm * normed, axis=-1, keepdims=True))


def chain_kernel(lens_ref, y1_ref, y2_ref, d1_ref, d2_ref, wup_ref, wdn_ref, wq_ref, wk_ref, wv_ref, wo_ref,
                 on1, oh, ou, oe, on2, oa, oc, odqkv, o_early, o_base, o_send, o_own,
                 w1, w2, wa, wo, n1b, eb, n2b, cb, hb, ub, ab, dqb, gp, qkv, pbuf,
                 part, rd, sx, rx, st,
                 s_in, s_w, s_out, s_ds, s_dr, s_xs, s_xr, s_as, s_ar, s_fin,
                 *, n_layers, seq, d_model, ff, nq, nkv, head_dim, n_chunk):
    tokens = 4 * seq
    cw = d_model // n_chunk
    fw = ff // n_chunk
    me = lax.axis_index("tp")
    xi = lax.div(me, 2)
    ci = lax.rem(me, 2)
    xo = 1 - xi
    co = 1 - ci
    x_dev = {"tp": 2 * xo + ci}
    c_dev = {"tp": 2 * xi + co}
    score_scale = head_dim ** -0.5

    def rows(slot):
        return pl.ds(pl.multiple_of(slot * seq, seq), seq)

    W_ATT = 2 * n_chunk
    W_OUT = W_ATT + 1

    def cols(k):
        return pl.ds(k * cw, cw)

    def w_copies(lay, group):
        if group < n_chunk:
            sl = pl.ds(group * fw, fw)
            return [pltpu.make_async_copy(wup_ref.at[lay, :, sl], w1.at[:, sl], s_w.at[group])]
        if group < 2 * n_chunk:
            return [pltpu.make_async_copy(wdn_ref.at[lay, :, cols(group - n_chunk)], w2.at[:, cols(group - n_chunk)],
                                          s_w.at[group])]
        if group == W_ATT:
            return [pltpu.make_async_copy(wq_ref.at[lay], wa.at[pl.ds(0, nq)], s_w.at[group]),
                    pltpu.make_async_copy(wk_ref.at[lay], wa.at[pl.ds(nq, nkv)], s_w.at[group + 2]),
                    pltpu.make_async_copy(wv_ref.at[lay], wa.at[pl.ds(nq + nkv, nkv)], s_w.at[group + 3])]
        return [pltpu.make_async_copy(wo_ref.at[lay], wo, s_w.at[group])]

    def w_start(lay, group):
        for cp in w_copies(lay, group):
            cp.start()

    def w_wait(lay, group):
        for cp in w_copies(lay, group):
            cp.wait()

    def d_copy(ty, k):
        return pltpu.make_async_remote_copy(
            part.at[ty, :, co, :, cols(k)], rd.at[ty, :, :, cols(k)], s_ds.at[ty, k], s_dr.at[ty, k],
            device_id=c_dev, device_id_type=MESH)

    def x_copy(ty, k):
        return pltpu.make_async_remote_copy(
            sx.at[ty, :, cols(k)], rx.at[ty, :, cols(k)], s_xs.at[ty, k], s_xr.at[ty, k],
            device_id=x_dev, device_id_type=MESH)

    def put_part(ty, k, val):
        part[ty, :, :, :, cols(k)] = val.reshape(2, 2, seq, cw)
        d_copy(ty, k).start()

    def mid(ty, k, send=None):
        d_copy(ty, k).wait_recv()
        sx[ty, :, cols(k)] = part[ty, xo, ci, :, cols(k)] + rd[ty, xo, :, cols(k)]
        if send is None:
            x_copy(ty, k).start()
        else:
            @pl.when(send)
            def _():
                x_copy(ty, k).start()

    def fin_sum(ty):
        for k in range(n_chunk):
            x_copy(ty, k).wait_recv()
        total = part[ty, xi, ci] + rd[ty, xi] + rx[ty]
        for k in range(n_chunk):
            x_copy(ty, k).wait_send()
            d_copy(ty, k).wait_send()
        return total

    ag_buf = {G: n2b, B: cb, FW: n1b, DW: eb}

    def ag_copy(ty, lay, step):
        buf = ag_buf[ty]
        slot = 2 * xo + ci if step == 2 else me
        return pltpu.make_async_remote_copy(
            buf.at[lay, rows(slot)], buf.at[lay, rows(slot)], s_as.at[ty, step], s_ar.at[ty, step],
            device_id=x_dev if step == 0 else c_dev, device_id_type=MESH)

    def ag_start(ty, lay, val):
        ag_buf[ty][lay, rows(me)] = val
        ag_copy(ty, lay, 0).start()
        ag_copy(ty, lay, 1).start()

    def ag_forward(ty, lay):
        ag_copy(ty, lay, 0).wait_recv()
        ag_copy(ty, lay, 2).start()

    def ag_ready(ty, lay):
        ag_copy(ty, lay, 1).wait_recv()
        ag_copy(ty, lay, 2).wait_recv()
        for step in range(3):
            ag_copy(ty, lay, step).wait_send()

    outs = [(on1, n1b), (oh, hb), (ou, ub), (oe, eb), (on2, n2b), (oa, ab), (oc, cb), (odqkv, dqb)]

    def out_copy(idx, lay):
        dst, src = outs[idx]
        return pltpu.make_async_copy(src.at[lay], dst.at[lay], s_out.at[idx, lay])

    def g_up(lay):
        for k in range(n_chunk):
            w_wait(lay, k)
            pre = dot_nn(n1b[lay], w1[:, pl.ds(k * fw, fw)])
            sq = pre * pre
            th = jnp.tanh(GELU_C * (pre + GELU_A * (sq * pre)))
            cdf = 0.5 * (1.0 + th)
            hb[lay, :, pl.ds(k * fw, fw)] = (pre * cdf).astype(BF16)
            gp[:, pl.ds(k * fw, fw)] = cdf + pre * (0.5 * (1.0 - th * th)) * (GELU_C * (1.0 + (3.0 * GELU_A) * sq))

    def g_put(lay, k):
        w_wait(lay, n_chunk + k)
        put_part(G, k, dot_nn(hb[lay], w2[:, cols(k)]))

    def b_up(lay, k):
        d_act = dot_nt(eb[lay], w2[pl.ds(k * fw, fw), :])
        ub[lay, :, pl.ds(k * fw, fw)] = (gp[:, pl.ds(k * fw, fw)] * d_act).astype(BF16)

    def b_put(lay, k):
        put_part(B, k, dot_nt(ub[lay], w1[cols(k), :]))

    lane = lax.broadcasted_iota(jnp.int32, (tokens, 2 * head_dim), 1)
    left = lane < head_dim

    def halves(blk):
        blk = blk.astype(F32)
        rolled = pltpu.roll(blk, head_dim, 1)
        zero = jnp.zeros_like(blk)
        return (((jnp.where(left, blk, zero)).astype(BF16), (jnp.where(left, zero, rolled)).astype(BF16)),
                ((jnp.where(left, rolled, zero)).astype(BF16), (jnp.where(left, zero, blk)).astype(BF16)))

    def visible():
        row = lax.broadcasted_iota(jnp.int32, (tokens, tokens), 0)
        col = lax.broadcasted_iota(jnp.int32, (tokens, tokens), 1)
        row_seq = lax.div(row, seq)
        limit = jnp.zeros((tokens, tokens), jnp.int32)
        for s in range(4):
            limit = jnp.where(row_seq == s, s * seq + lens_ref[s], limit)
        return (col <= row) & (col >= row_seq * seq) & (col < limit)

    n_pairs = nq // (2 * head_dim)
    pairs_per_slot = n_pairs // 2

    def f_proj(lay):
        qkv[...] = dot_nt(n2b[lay], wa[...]).astype(BF16)

    def f_attn(lay):
        keys = halves(qkv[:, nq:nq + nkv])
        vals = halves(qkv[:, nq + nkv:])
        vis = visible()
        for j in range(n_pairs):
            slot = j // pairs_per_slot
            q_pair = qkv[:, j * 2 * head_dim:(j + 1) * 2 * head_dim]
            att = None
            for half in range(2):
                s_val = jnp.where(vis, dot_nt(q_pair, keys[slot][half]) * score_scale, MASK_VALUE)
                ex = jnp.exp(s_val - jnp.max(s_val, axis=-1, keepdims=True))
                prob = ex / jnp.sum(ex, axis=-1, keepdims=True)
                pbuf[2 * j + half] = prob
                term = dot_nn(prob.astype(BF16), vals[slot][half])
                att = term if att is None else att + term
            ab[lay, :, j * 2 * head_dim:(j + 1) * 2 * head_dim] = att.astype(BF16)

    def f_put(lay, k):
        put_part(FW, k, dot_nn(ab[lay], wo[:, cols(k)]))

    def d_attn(lay):
        d_out = dot_nt(cb[lay], wo[...]).astype(BF16)
        keys = halves(qkv[:, nq:nq + nkv])
        vals = halves(qkv[:, nq + nkv:])
        acc_v = [[None, None], [None, None]]
        acc_k = [[None, None], [None, None]]
        for j in range(n_pairs):
            slot = j // pairs_per_slot
            sl = slice(j * 2 * head_dim, (j + 1) * 2 * head_dim)
            q_pair = qkv[:, sl]
            d_pair = d_out[:, sl]
            dq = None
            for half in range(2):
                prob = pbuf[2 * j + half]
                tv = dot_tn(prob.astype(BF16), d_pair)
                dp = dot_nt(d_pair, vals[slot][half])
                row_dot = jnp.sum(prob * dp, axis=-1, keepdims=True)
                ds = (prob * (dp - row_dot) * score_scale).astype(BF16)
                tk = dot_tn(ds, q_pair)
                tq = dot_nn(ds, keys[slot][half])
                dq = tq if dq is None else dq + tq
                prev = acc_v[slot][half]
                acc_v[slot][half] = tv if prev is None else prev + tv
                prev = acc_k[slot][half]
                acc_k[slot][half] = tk if prev is None else prev + tk
            dqb[lay, :, sl] = dq.astype(BF16)

        def merge(acc):
            slot0 = acc[0][0] + pltpu.roll(acc[0][1], head_dim, 1)
            slot1 = pltpu.roll(acc[1][0], head_dim, 1) + acc[1][1]
            return jnp.where(left, slot0, slot1).astype(BF16)

        dqb[lay, :, nq:nq + nkv] = merge(acc_k)
        dqb[lay, :, nq + nkv:] = merge(acc_v)

    def d_put(lay, k):
        put_part(DW, k, dot_nn(dqb[lay], wa[:, cols(k)]))

    def g_fin(lay):
        x2 = st[2] - fin_sum(G)
        st[2] = x2
        ag_start(G, lay, (x2 * inv_rms(x2)).astype(BF16))

    def b_fin(lay):
        dy1 = st[3] + rms_back(st[0], fin_sum(B))
        st[3] = dy1
        ag_start(B, lay, dy1.astype(BF16))

    def f_fin(lay):
        x1 = st[0] - fin_sum(FW)
        st[0] = x1
        ag_start(FW, lay - 1, (x1 * inv_rms(x1)).astype(BF16))

    def d_fin(lay):
        dx2 = st[1] + rms_back(st[2], fin_sum(DW))
        st[1] = dx2
        ag_start(DW, lay - 1, dx2.astype(BF16))

    top = n_layers - 1
    in_full = [pltpu.make_async_copy(y1_ref, part.at[FW], s_in.at[0]),
               pltpu.make_async_copy(d2_ref, part.at[DW], s_in.at[1])]
    in_own = [pltpu.make_async_copy(src.at[xi, ci], st.at[i], s_in.at[2 + i])
              for i, src in enumerate((y1_ref, d2_ref, y2_ref, d1_ref))]
    in_full[0].start()
    for k in range(2 * n_chunk):
        w_start(top, k)
    in_full[1].start()
    for cp in in_own:
        cp.start()
    w_start(top, W_ATT)
    w_start(top, W_OUT)
    barrier = pltpu.get_barrier_semaphore()
    pl.semaphore_signal(barrier, inc=1, device_id=x_dev, device_id_type=MESH)
    pl.semaphore_signal(barrier, inc=1, device_id=c_dev, device_id_type=MESH)
    in_full[0].wait()
    for a in range(2):
        for b in range(2):
            y_val = part[FW, a, b]
            n1b[top, pl.ds((2 * a + b) * seq, seq)] = (y_val * inv_rms(y_val)).astype(BF16)
    pl.semaphore_wait(barrier, 2)

    def layer_body(i, carry):
        lay = top - i
        more = i < top
        first = i == 0
        later = i > 0

        @pl.when(later)
        def _():
            f_fin(lay + 1)
            d_fin(lay + 1)
            ag_forward(FW, lay)
            ag_ready(FW, lay)

        g_up(lay)
        out_copy(0, lay).start()
        out_copy(1, lay).start()
        g_put(lay, 0)

        @pl.when(later)
        def _():
            ag_forward(DW, lay)

        g_put(lay, 1)
        g_put(lay, 2)
        mid(G, 0)
        g_put(lay, 3)
        mid(G, 1)

        @pl.when(later)
        def _():
            ag_ready(DW, lay)

        @pl.when(first)
        def _():
            in_full[1].wait()
            for a in range(2):
                for b in range(2):
                    eb[top, pl.ds((2 * a + b) * seq, seq)] = part[DW, a, b].astype(BF16)
            for cp in in_own:
                cp.wait()

        b_up(lay, 0)
        mid(G, 2)
        mid(G, 3)
        for k in range(1, n_chunk):
            b_up(lay, k)
        out_copy(2, lay).start()
        out_copy(3, lay).start()
        b_put(lay, 0)
        b_put(lay, 1)
        mid(B, 0)
        b_put(lay, 2)
        b_put(lay, 3)

        @pl.when(more)
        def _():
            for k in range(2 * n_chunk):
                w_start(lay - 1, k)

        mid(B, 1)
        g_fin(lay)
        mid(B, 2)
        mid(B, 3)
        ag_forward(G, lay)
        b_fin(lay)
        ag_ready(G, lay)
        out_copy(4, lay).start()
        w_wait(lay, W_ATT)
        f_proj(lay)
        f_attn(lay)
        out_copy(5, lay).start()
        w_wait(lay, W_OUT)
        f_put(lay, 0)
        f_put(lay, 1)
        f_put(lay, 2)
        f_put(lay, 3)
        mid(FW, 0, more)
        mid(FW, 1, more)
        ag_forward(B, lay)
        mid(FW, 2, more)
        mid(FW, 3, more)
        ag_ready(B, lay)
        out_copy(6, lay).start()
        d_attn(lay)
        out_copy(7, lay).start()
        for k in range(n_chunk):
            d_put(lay, k)

        @pl.when(more)
        def _():
            w_start(lay - 1, W_ATT)
            w_start(lay - 1, W_OUT)

        for k in range(n_chunk):
            mid(DW, k, more)
        return carry

    lax.fori_loop(0, n_layers, layer_body, 0)
    for ty in (FW, DW):
        rx[ty] = part[ty, xi, ci] + rd[ty, xi]
    tail = [pltpu.make_async_copy(src, dst, s_fin.at[i]) for i, (src, dst) in enumerate(
        ((st.at[pl.ds(2, 2)], o_early), (st.at[pl.ds(0, 2)], o_base),
         (sx.at[pl.ds(FW, 2)], o_send), (rx.at[pl.ds(FW, 2)], o_own)))]
    for cp in tail:
        cp.start()
    for ty in (FW, DW):
        for k in range(n_chunk):
            d_copy(ty, k).wait_send()
    for idx in range(8):
        for lay in range(n_layers):
            out_copy(idx, lay).wait()
    for cp in tail:
        cp.wait()


def run_chain(lens, y1, y2, d1, d2, w_up, w_down, wq, wk, wv, wo):
    n_layers, d_model, ff = w_up.shape
    seq = y1.shape[2]
    tokens = 4 * seq
    nq, nkv = wq.shape[1], wk.shape[1]
    head_dim = nkv // 2
    n_chunk = 4
    n_w = nq + 2 * nkv
    body = functools.partial(chain_kernel, n_layers=n_layers, seq=seq, d_model=d_model, ff=ff, nq=nq, nkv=nkv,
                             head_dim=head_dim, n_chunk=n_chunk)
    any_spec = pl.BlockSpec(memory_space=pl.ANY)
    wide = jax.ShapeDtypeStruct((n_layers, tokens, d_model), BF16)
    wide_ff = jax.ShapeDtypeStruct((n_layers, tokens, ff), BF16)
    out_shape = [wide, wide_ff, wide_ff, wide, wide, jax.ShapeDtypeStruct((n_layers, tokens, nq), BF16), wide,
                 jax.ShapeDtypeStruct((n_layers, tokens, n_w), BF16),
                 ] + [jax.ShapeDtypeStruct((2, seq, d_model), F32)] * 4
    vm = pltpu.VMEM
    dma = pltpu.SemaphoreType.DMA
    scratch = [vm((d_model, ff), BF16), vm((ff, d_model), BF16), vm((n_w, d_model), BF16), vm((nq, d_model), BF16),
               vm((n_layers, tokens, d_model), BF16), vm((n_layers, tokens, d_model), BF16),
               vm((n_layers, tokens, d_model), BF16), vm((n_layers, tokens, d_model), BF16),
               vm((n_layers, tokens, ff), BF16), vm((n_layers, tokens, ff), BF16),
               vm((n_layers, tokens, nq), BF16), vm((n_layers, tokens, n_w), BF16),
               vm((tokens, ff), F32), vm((tokens, n_w), BF16), vm((nq // head_dim, tokens, tokens), F32),
               vm((4, 2, 2, seq, d_model), F32), vm((4, 2, seq, d_model), F32),
               vm((4, seq, d_model), F32), vm((4, seq, d_model), F32), vm((4, seq, d_model), F32),
               dma((6,)), dma((2 * n_chunk + 4,)), dma((8, n_layers)),
               dma((4, n_chunk)), dma((4, n_chunk)), dma((4, n_chunk)), dma((4, n_chunk)),
               dma((4, 3)), dma((4, 3)), dma((4,))]
    return pl.pallas_call(
        body, out_shape=out_shape,
        in_specs=[pl.BlockSpec(memory_space=pltpu.SMEM)] + [any_spec] * 10,
        out_specs=[any_spec] * 12,
        scratch_shapes=scratch,
        compiler_params=pltpu.CompilerParams(collective_id=0, has_side_effects=True, vmem_limit_bytes=60 * 2 ** 20),
        cost_estimate=pl.CostEstimate(flops=60 * 10 ** 9, bytes_accessed=10 ** 8, transcendentals=0),
        name="chain",
    )(lens, y1, y2, d1, d2, w_up, w_down, wq, wk, wv, wo)


def grad_kernel(*refs, nq, nkv, n_tiles, start, n_prev):
    n1_ref, u_ref, h_ref, e_ref, dqkv_ref, n2_ref, a_ref, c_ref = refs[:8]
    pos = 8 + n_prev
    dup_ref, ddn_ref, dq_ref, dk_ref, dv_ref, do_ref = refs[pos:pos + 6]
    idx = pl.program_id(0)
    step = lax.rem(idx + start, n_tiles)
    dup_ref[0] = dot_tn(n1_ref[0], u_ref[0])
    ddn_ref[0] = dot_tn(h_ref[0], e_ref[0])
    tile = pl.ds(pl.multiple_of(lax.div(step, 2) * 128, 128), 128)

    @pl.when(lax.rem(step, 2) == 0)
    def _():
        dq_ref[0] = dot_tn(dqkv_ref[0, :, tile], n2_ref[0])

    @pl.when(lax.rem(step, 2) == 1)
    def _():
        do_ref[0] = dot_tn(a_ref[0, :, tile], c_ref[0])

    @pl.when(step == 1)
    def _():
        dk_ref[0] = dot_tn(dqkv_ref[0, :, nq:nq + nkv], n2_ref[0])

    @pl.when(step == 4)
    def _():
        dv_ref[0] = dot_tn(dqkv_ref[0, :, nq + nkv:], n2_ref[0])


def weight_grads(ops, start, count, nq, nkv, prev=None):
    n1, u, h, e, dqkv, n2, a, c = ops
    n_layers, tokens, d_model = n1.shape
    ff = u.shape[2]
    n_tiles = 2 * nq // 128
    rd, rf = d_model // n_tiles, ff // n_tiles
    n_w = nq + 2 * nkv

    def lay(i):
        return (i + start) // n_tiles

    def tile_of(i):
        return (i + start) % n_tiles

    def full(width):
        return pl.BlockSpec((1, tokens, width), lambda i: (lay(i), 0, 0))

    def tile(width):
        return pl.BlockSpec((1, tokens, width), lambda i: (lay(i), 0, tile_of(i)))

    def rows(n_rows, width):
        return pl.BlockSpec((1, n_rows, width), lambda i: (lay(i), tile_of(i), 0))

    def half(n_rows, width):
        return pl.BlockSpec((1, n_rows, width), lambda i: (lay(i), tile_of(i) // 2, 0))

    def whole(n_rows, width):
        return pl.BlockSpec((1, n_rows, width), lambda i: (lay(i), 0, 0))

    in_specs = [tile(rd), full(ff), tile(rf), full(d_model), full(n_w), full(d_model), full(nq), full(d_model)]
    operands = list(ops)
    any_spec = pl.BlockSpec(memory_space=pl.ANY)
    out_shape = [jax.ShapeDtypeStruct((n_layers, r, w), F32)
                 for r, w in ((d_model, ff), (ff, d_model), (nq, d_model), (nkv, d_model), (nkv, d_model), (nq, d_model))]
    out_specs = [rows(rd, ff), rows(rf, d_model), half(128, d_model), whole(nkv, d_model), whole(nkv, d_model),
                 half(128, d_model)]
    aliases = {}
    if prev is not None:
        aliases = {len(operands) + i: i for i in range(6)}
        operands += list(prev)
        in_specs += [any_spec] * 6
    return pl.pallas_call(
        functools.partial(grad_kernel, nq=nq, nkv=nkv, n_tiles=n_tiles, start=start,
                          n_prev=6 if prev is not None else 0),
        grid=(count,), out_shape=out_shape, in_specs=in_specs, out_specs=out_specs,
        input_output_aliases=aliases,
        compiler_params=pltpu.CompilerParams(dimension_semantics=("arbitrary",)),
        cost_estimate=pl.CostEstimate(flops=10 ** 9 * count, bytes_accessed=6 * 10 ** 6 * count, transcendentals=0),
        name="weight_grads",
    )(*operands)


def last_kernel(base_ref, early_ref, own_ref, got_ref, fin_ref):
    fin_ref[0] = base_ref[0] - (own_ref[0] + got_ref[0])
    fin_ref[1] = early_ref[0]
    fin_ref[2] = early_ref[1]
    fin_ref[3] = base_ref[1] + rms_back(early_ref[0], own_ref[1] + got_ref[1])


def last_sums(base, early, own, got):
    vmem = pl.BlockSpec(memory_space=pltpu.VMEM)
    return pl.pallas_call(
        last_kernel, out_shape=jax.ShapeDtypeStruct((4,) + base.shape[1:], F32), in_specs=[vmem] * 4, out_specs=vmem,
        compiler_params=pltpu.CompilerParams(vmem_limit_bytes=8 * 2 ** 20), name="last_sums",
    )(base, early, own, got)


def place_kernel(*refs):
    srcs, out_refs, sems = refs[:4], refs[4:8], refs[8]
    me = lax.axis_index("tp")
    xi, ci = lax.div(me, 2), lax.rem(me, 2)
    slots = (me, 2 * (1 - xi) + ci, 2 * xi + 1 - ci, 2 * (1 - xi) + 1 - ci)
    copies = [pltpu.make_async_copy(srcs[i].at[j], out_refs[j].at[slots[i]], sems.at[i, j])
              for i in range(4) for j in range(4)]
    for cp in copies:
        cp.start()
    for cp in copies:
        cp.wait()


def place(*parts):
    _, seq, d_model = parts[0].shape
    return pl.pallas_call(
        place_kernel, out_shape=[jax.ShapeDtypeStruct((4, seq, d_model), F32)] * 4,
        in_specs=[pl.BlockSpec(memory_space=pltpu.VMEM)] * 4, out_specs=[pl.BlockSpec(memory_space=pl.ANY)] * 4,
        scratch_shapes=[pltpu.SemaphoreType.DMA((4, 4))],
        compiler_params=pltpu.CompilerParams(vmem_limit_bytes=16 * 2 ** 20), name="place",
    )(*parts)


def solution(mesh):
    act_spec = P('dp', None, None)
    w_specs = (P(None, None, 'tp', None), P(None, None, 'tp', None), P(None, None, 'tp', None),
               P(None, 'tp', None, None), P(None, None, 'tp'), P(None, 'tp', None))
    g_specs = (P('dp', None, 'tp', None), P('dp', None, 'tp', None), P('dp', None, 'tp', None),
               P('dp', 'tp', None, None), P('dp', None, 'tp'), P('dp', 'tp', None))

    def local_fn(y_one, y_two, dy_one, dy_two, seq_lens, w_query, w_key, w_value, w_out, w_up, w_down):
        n_layers, d_model, heads, head_dim = w_query.shape
        slots = w_key.shape[2]
        seq = y_one.shape[1]
        nq, nkv = heads * head_dim, slots * head_dim

        def to_rows(w, width):
            return jnp.transpose(w, (0, 2, 3, 1)).reshape(n_layers, width, d_model)

        def from_rows(g, n_heads):
            return jnp.transpose(g.reshape(n_layers, n_heads, head_dim, d_model), (0, 3, 1, 2))

        acts = [a.reshape(2, 2, seq, d_model) for a in (y_one, y_two, dy_one, dy_two)]
        n1, h, u, e, n2, a, c, dqkv, early, base, send, own = run_chain(
            seq_lens, *acts, w_up, w_down, to_rows(w_query, nq), to_rows(w_key, nkv), to_rows(w_value, nkv),
            w_out.reshape(n_layers, nq, d_model))
        ops = (n1, u, h, e, dqkv, n2, a, c)
        chips = [(0, 2), (2, 0), (1, 3), (3, 1)]
        cores = [(0, 1), (1, 0), (2, 3), (3, 2)]
        got = lax.ppermute(send, "tp", chips)
        n_tiles = 2 * nq // 128

        def tie(grads, *vals):
            tied = lax.optimization_barrier((grads[3],) + vals)
            return list(grads[:3]) + [tied[0]] + list(grads[4:]), tied[1:]

        grads = weight_grads(ops, 0, n_tiles, nq, nkv)
        grads, (got,) = tie(grads, got)
        fin = last_sums(base, early, own, got)
        grads, (fin,) = tie(grads, fin)
        across = lax.ppermute(fin, "tp", chips)
        near = lax.ppermute(fin, "tp", cores)
        grads = weight_grads(ops, n_tiles, (n_layers - 1) * n_tiles, nq, nkv, prev=grads)
        grads, (across,) = tie(grads, across)
        far = lax.ppermute(across, "tp", cores)
        d_up, d_down, dq, dk, dv, do = grads
        outs = [o.reshape(y_one.shape) for o in place(fin, across, near, far)]
        return (outs[0], outs[1], outs[2], outs[3],
                from_rows(dq, heads), from_rows(dk, slots), from_rows(dv, slots),
                do.reshape(n_layers, heads, head_dim, d_model), d_up, d_down)

    return jax.shard_map(local_fn, mesh=mesh,
                         in_specs=(act_spec,) * 4 + (P('dp'),) + w_specs,
                         out_specs=(act_spec,) * 4 + g_specs,
                         check_vma=False)
```
